512 devices in a mesh: gx: 16 (over z, core), gy: 4 (over x), gz: 8 (over y).
Axes of the slice: x: 4, y: 8, z: 8, core: 2. Of those that a mesh axis runs over, the one named last changes fastest.
Arguments:
- krylov_basis: float32 [60, 64, 32, 1024], P(None, 'gx', 'gy', 'gz'), may hold values from -6 to 6
- schur_vectors: float32 [60, 20], replicated, may hold values from -1 to 1, as said below
- next_vector: float32 [64, 32, 1024], P('gx', 'gy', 'gz'), may hold values from -10 to 10
- diag_shift: float32 [64, 32, 1024], P('gx', 'gy', 'gz'), may hold values from 0.25 to 2
- velocity: float32 [3, 64, 32, 1024], P(None, 'gx', 'gy', 'gz'), may hold values from -1 to 1
Outputs:
- new_basis: float32 [24, 64, 32, 1024], P(None, 'gx', 'gy', 'gz')
- hessenberg: float32 [24, 3], replicated
The draws below stay inside these ranges and needn't reach their ends.
Inputs may be any that keep to these rules, and one draw needn't show every extreme that they name: `schur_vectors`: the columns are orthonormal.
All inputs are finite; a program needn't handle non-finite values.
Results may differ from the reference program's by a relative error of at most 0.0003.
Values sent between devices are 32-bit elements; how exact they have to be, the bound alone decides.
A program may use at most 64 MiB of HBM per device.

```python
import jax
import jax.numpy as jnp
from jax import lax

BASIS = 60
KEEP = 20
EXPAND = 3
ROWS = 24
NX = 64
NY = 32
NZ = 1024


def draw_schur_vectors(key, part):
    gaussian = jax.random.normal(key, (BASIS, KEEP), jnp.float32)
    orthonormal, triangle = jnp.linalg.qr(gaussian)
    return orthonormal.astype(jnp.float32)


def levels(stream_key, shape, split, least, largest):
    level = 1.0
    for axis_at, parts in split:
        heights = jax.random.uniform(jax.random.fold_in(jax.random.fold_in(stream_key, 6), axis_at), (parts,), jnp.float32, least / len(split), largest / len(split))
        level = level * jnp.repeat(jnp.exp(heights), shape[axis_at] // parts).reshape((-1,) + (1,) * (len(shape) - 1 - axis_at))
    return level


def noise(key, extent, scale, bound, shards=(), dtype=jnp.bfloat16):
    factor_of = levels(key, extent, shards, -0.22, 0.18) if shards else 1.0
    entries = jax.random.normal(key, extent, jnp.float32) * scale * factor_of
    return jnp.minimum(jnp.maximum(entries, -bound), bound).astype(dtype)


def setup_inputs(seed: int = 0) -> dict:
    key_list = jax.random.split(jax.random.key(seed), 6)
    krylov_basis = noise(key_list[0], (BASIS, NX, NY, NZ), 1.0, 6.0, ((1, 16), (2, 4), (3, 8)), jnp.float32)
    schur_vectors = draw_schur_vectors(jax.random.fold_in(key_list[5], 71), 0)
    next_vector = noise(key_list[2], (NX, NY, NZ), 2.0, 10.0, ((0, 16), (1, 4), (2, 8)), jnp.float32)
    diag_shift = jnp.clip(0.25 + 1.75 * jax.random.uniform(key_list[3], (NX, NY, NZ), jnp.float32) ** levels(key_list[3], (NX, NY, NZ), ((0, 16), (1, 4), (2, 8)), -0.2, 0.2), 0.25, 2.0)
    velocity = jnp.clip(jax.random.uniform(key_list[4], (3, NX, NY, NZ), jnp.float32, -1.0, 1.0) * levels(key_list[4], (3, NX, NY, NZ), ((1, 16), (2, 4), (3, 8)), -0.4, 0.0), -1.0, 1.0)
    return {"krylov_basis": krylov_basis, "schur_vectors": schur_vectors, "next_vector": next_vector, "diag_shift": diag_shift, "velocity": velocity}


def operate_field(field, diag_shift, velocity):
    padded = jnp.pad(field, 1)
    x_ahead = padded[2:, 1:-1, 1:-1]
    x_behind = padded[:-2, 1:-1, 1:-1]
    y_ahead = padded[1:-1, 2:, 1:-1]
    y_behind = padded[1:-1, :-2, 1:-1]
    z_ahead = padded[1:-1, 1:-1, 2:]
    z_behind = padded[1:-1, 1:-1, :-2]
    neighbours = x_ahead + x_behind + y_ahead + y_behind + z_ahead + z_behind
    flow = velocity[0] * (x_ahead - x_behind) + velocity[1] * (y_ahead - y_behind) + velocity[2] * (z_ahead - z_behind)
    return (6.0 + diag_shift) * field - neighbours + 0.5 * flow

def reference(krylov_basis, schur_vectors, next_vector, diag_shift, velocity):
    highest = lax.Precision.HIGHEST
    cell_count = NX * NY * NZ
    rotated = jnp.einsum('ik,ixyz->kxyz', schur_vectors, krylov_basis, precision=highest)
    norm_sq = jnp.sum(next_vector * next_vector) / cell_count
    first = next_vector / jnp.maximum(jnp.sqrt(norm_sq), 0.5)
    vectors = jnp.concatenate([rotated, first[None]], axis=0)
    columns = []
    for expansion in range(EXPAND):
        count = vectors.shape[0]
        flat_basis = vectors.reshape(count, -1)
        applied = operate_field(vectors[-1], diag_shift, velocity).reshape(-1)
        first_coeffs = jnp.dot(flat_basis, applied, precision=highest) / cell_count
        partly = applied - jnp.dot(first_coeffs, flat_basis, precision=highest)
        second_coeffs = jnp.dot(flat_basis, partly, precision=highest) / cell_count
        cleaned = partly - jnp.dot(second_coeffs, flat_basis, precision=highest)
        length = jnp.sqrt(jnp.sum(cleaned * cleaned) / cell_count)
        column = jnp.zeros((ROWS,), jnp.float32)
        column = column.at[:count].set(first_coeffs + second_coeffs).at[count].set(length)
        columns.append(column)
        newest = (cleaned / jnp.maximum(length, 0.5)).reshape(NX, NY, NZ)
        vectors = jnp.concatenate([vectors, newest[None]], axis=0)
    return (vectors, jnp.stack(columns, axis=1))
```

```python
import functools

import jax
import jax.numpy as jnp
from jax import lax
from jax.experimental import pallas as pl
from jax.experimental.pallas import tpu as pltpu
from jax.sharding import PartitionSpec as P

KEEP = 20
EXPAND = 3
ROWS = 24
LANES = 128
UNIT = 16
PITCH = 40
AXES = ("gx", "gy", "gz")


def partner_steps(phase, sizes):
    if phase == 1:
        return [(dx, 0, 0) for dx in range(1, sizes[0])]
    return [(0, dy, dz) for dy in range(sizes[1]) for dz in range(sizes[2])][1:]


def body(
    sizes, cells,
    kry_hbm, schur_hbm, w_hbm, diag_hbm, vel_hbm,
    out, hess,
    schur, w_ref, diag, vel, kry, coef, t0, t1, t2, wrow, image,
    xs, ys, zs, xh, yh, zh, zpack, split0, split1,
    gsend, grecv0, grecv1, bsend, brecv0, brecv1, rsend, rrecv0, rrecv1,
    load_sem, halo_send, halo_recv, red_send, red_recv,
):
    f32, bf16 = jnp.float32, jnp.bfloat16
    place = tuple(lax.axis_index(a) for a in AXES)
    basis = kry_hbm.shape[0]
    bx, by, bz = w_ref.shape
    area = bx * by
    loads = [
        pltpu.make_async_copy(source, target, load_sem.at[k])
        for k, (source, target) in enumerate((
            (w_hbm, w_ref), (kry_hbm, kry_hbm), (schur_hbm, schur),
            (diag_hbm, diag), (vel_hbm, vel)))
    ]
    for copy in loads[:1] + loads[2:]:
        copy.start()
    for i in range(basis):
        pltpu.make_async_copy(
            kry_hbm.at[i], kry.at[pl.ds(i * PITCH, area)], load_sem.at[1]).start()
    shifted = [[lax.rem(place[d] + k, sizes[d]) for k in range(sizes[d])] for d in range(3)]

    def partners(phase):
        return [tuple(shifted[d][step[d]] for d in range(3))
                for step in partner_steps(phase, sizes)]

    barrier = pltpu.get_barrier_semaphore()
    for to in partners(0) + partners(1):
        pl.semaphore_signal(
            barrier, inc=1, device_id=to, device_id_type=pl.DeviceIdType.MESH)

    for d, slots in enumerate(((xs, xh), (ys, yh), (zs, zh))):
        for side in (0, 1):
            def clear(slots=slots, side=side):
                for ref in slots:
                    for k in range(ref.shape[0]):
                        ref[k, side] = jnp.zeros(ref.shape[2:], f32)
            pl.when(place[d] == (0 if side == 0 else sizes[d] - 1))(clear)

    def halo_copies(kind, sources, targets):
        found = []
        for d in range(3):
            for side in (0, 1):
                at = (kind * 3 + d) * 2 + side
                to = list(place)
                to[d] = place[d] + (1 if side == 0 else -1)
                can_send = place[d] < sizes[d] - 1 if side == 0 else place[d] > 0
                can_recv = place[d] > 0 if side == 0 else place[d] < sizes[d] - 1
                found.append((
                    pltpu.make_async_remote_copy(
                        src_ref=sources[d][side], dst_ref=targets[d][side],
                        send_sem=halo_send.at[at], recv_sem=halo_recv.at[at],
                        device_id=tuple(to), device_id_type=pl.DeviceIdType.MESH,
                    ), can_send, can_recv))
        return found

    def halo_start(copies):
        for copy, can_send, _ in copies:
            pl.when(can_send)(copy.start)

    def halo_wait(copies):
        for copy, _, can_recv in copies:
            pl.when(can_recv)(copy.wait_recv)

    def halo_finish(copies):
        for copy, can_send, _ in copies:
            pl.when(can_send)(copy.wait_send)

    def field_copies(kind, ref):
        return halo_copies(
            kind,
            ((ref.at[bx - 1], ref.at[0]), (ref, ref), (ref, ref)),
            tuple((r.at[kind, 0], r.at[kind, 1]) for r in (xs, ys, zs)),
        )

    def rows_copies(level, ref):
        return halo_copies(
            EXPAND + level,
            ((ref.at[bx - 1], ref.at[0]), (ref.at[:, by - 1], ref.at[:, 0]),
             (zpack.at[level, 0], zpack.at[level, 1])),
            tuple((r.at[level, 0], r.at[level, 1]) for r in (xh, yh, zh)),
        )

    pending = []

    def exchange(kind, send, slots, phase):
        at = kind * 2 + phase
        for k, to in enumerate(partners(phase)):
            pltpu.make_async_remote_copy(
                src_ref=send, dst_ref=slots.at[k], send_sem=red_send.at[at],
                recv_sem=red_recv.at[at],
                device_id=to, device_id_type=pl.DeviceIdType.MESH,
            ).start()
        pending.append(pltpu.make_async_copy(slots, slots, red_send.at[at]))
        return pltpu.make_async_copy(slots, slots, red_recv.at[at])

    def gather_sum(arrival, own, slots):
        arrival.wait()
        terms = [own] + [slots[k] for k in range(slots.shape[0])]
        while len(terms) > 1:
            terms = [sum(terms[k + 1:k + 2], terms[k]) for k in range(0, len(terms), 2)]
        return terms[0]

    def reduce_start(kind, buffers, value):
        send, slots0, _ = buffers
        send[0] = value
        return value, exchange(kind, send.at[0], slots0, 0)

    def reduce_turn(kind, buffers, state):
        send, slots0, slots1 = buffers
        value = gather_sum(state[1], state[0], slots0)
        send[1] = value
        return value, exchange(kind, send.at[1], slots1, 1)

    def reduce_end(buffers, state):
        return gather_sum(state[1], state[0], buffers[2]) * (1.0 / cells)

    gram_buffers = (gsend, grecv0, grecv1)
    back_buffers = (bsend, brecv0, brecv1)
    row_buffers = (rsend, rrecv0, rrecv1)

    lane3 = lax.broadcasted_iota(jnp.int32, (by, bz), 1)
    row3 = lax.broadcasted_iota(jnp.int32, (by, bz), 0)
    lane24 = lax.broadcasted_iota(jnp.int32, (ROWS, bz), 1)

    def field_stencil(v, kind):
        res = []
        for x in range(bx):
            here = v[x]
            xb = v[x - 1] if x > 0 else xs[kind, 0]
            xa = v[x + 1] if x < bx - 1 else xs[kind, 1]
            yb = jnp.where(row3 == 0, ys[kind, 0, x, by - 1:by, :], pltpu.roll(here, 1, 0))
            ya = jnp.where(row3 == by - 1, ys[kind, 1, x, 0:1, :], pltpu.roll(here, by - 1, 0))
            zb = jnp.where(lane3 == 0, zs[kind, 0, x, :, bz - 1:bz], pltpu.roll(here, 1, 1))
            za = jnp.where(lane3 == bz - 1, zs[kind, 1, x, :, 0:1], pltpu.roll(here, bz - 1, 1))
            res.append(coef[6, x] * here + (coef[0, x] * xb + coef[1, x] * xa)
                       + (coef[2, x] * yb + coef[3, x] * ya)
                       + (coef[4, x] * zb + coef[5, x] * za))
        return res

    def rows_stencil(level, source, target):
        low, high = zh[level, 0], zh[level, 1]
        for x in range(bx):
            for y in range(by):
                at = x * by + y
                here = source[x, y]
                xb = source[x - 1, y] if x > 0 else xh[level, 0, y]
                xa = source[x + 1, y] if x < bx - 1 else xh[level, 1, y]
                yb = source[x, y - 1] if y > 0 else yh[level, 0, x]
                ya = source[x, y + 1] if y < by - 1 else yh[level, 1, x]
                zb = jnp.where(lane24 == 0, pltpu.roll(low, (bz - at) % bz, 1),
                               pltpu.roll(here, 1, 1))
                za = jnp.where(lane24 == bz - 1, pltpu.roll(high, bz - 1 - at, 1),
                               pltpu.roll(here, bz - 1, 1))
                c = [coef[k, x, y:y + 1, :] for k in range(7)]
                target[x, y] = (c[6] * here + (c[0] * xb + c[1] * xa)
                                + (c[2] * yb + c[3] * ya) + (c[4] * zb + c[5] * za))

    def pack_faces(level, source):
        for side, edge in enumerate((bz - 1, 0)):
            face = jnp.zeros((ROWS, bz), f32)
            for x in range(bx):
                for y in range(by):
                    at = x * by + y
                    face = jnp.where(
                        lane24 == at, pltpu.roll(source[x, y], (at - edge) % bz, 1), face)
            zpack[level, side] = face

    def put_row(k, tiles):
        for x in range(bx):
            wrow[pl.ds(x * by * 8 + 4 + k, by, stride=8), :] = tiles[x]

    def tail(x, y):
        return t0[x, y, 16:24] + wrow[(x * by + y) * 8:(x * by + y) * 8 + 8]

    def first_block(x, y):
        return [t0[x, y, 0:8], t0[x, y, 8:16], tail(x, y)]

    def second_block(x, y):
        return [t1[x, y, 0:8], t1[x, y, 8:16], t1[x, y, 16:24]]

    def put_split(ref, p, u):
        n = u.shape[0]
        at = pl.ds(p * 2 * bz, 2 * bz)
        high = u.astype(bf16)
        rest = u - high.astype(f32)
        mid = rest.astype(bf16)
        ref[0:n, at] = high
        ref[n:2 * n, at] = mid
        ref[2 * n:3 * n, at] = (rest - mid.astype(f32)).astype(bf16)

    def both(block, p):
        return [jnp.concatenate([block(*divmod(2 * p, by))[k], block(*divmod(2 * p + 1, by))[k]],
                                axis=1) for k in range(3)]

    dot_nt = functools.partial(
        lax.dot_general, dimension_numbers=(((1,), (1,)), ((), ())), preferred_element_type=f32)

    halo_w = field_copies(0, w_ref)
    wrow[...] = jnp.zeros_like(wrow)
    t0[:, :, 16:24] = jnp.zeros((bx, by, 8, bz), f32)
    split0[96:128] = jnp.zeros((32, split0.shape[1]), bf16)
    loads[0].wait()
    pl.semaphore_wait(barrier, len(partners(0)) + len(partners(1)))
    halo_start(halo_w)
    w = [w_ref[x] for x in range(bx)]
    put_row(0, w)

    loads[2].wait()
    loads[1].wait()
    turn = schur[...]
    turn_high = turn.astype(bf16)
    turn_low = (turn - turn_high.astype(f32)).astype(bf16)
    for p in range(area // 2):
        u = jnp.concatenate([kry[pl.ds(2 * p, basis, stride=PITCH), :],
                             kry[pl.ds(2 * p + 1, basis, stride=PITCH), :]], axis=1)
        high = u.astype(bf16)
        low = (u - high.astype(f32)).astype(bf16)
        r = (jnp.dot(turn_high, high, preferred_element_type=f32)
             + (jnp.dot(turn_high, low, preferred_element_type=f32)
                + jnp.dot(turn_low, high, preferred_element_type=f32)))
        for k in (0, 1):
            x, y = divmod(2 * p + k, by)
            t0[x, y, 0:KEEP] = r[:, k * bz:(k + 1) * bz]
    pack_faces(0, t0)
    halo_r = rows_copies(0, t0)
    halo_start(halo_r)

    loads[3].wait()
    loads[4].wait()
    for x in range(bx):
        for d in range(3):
            half = 0.5 * vel[d, x]
            coef[2 * d, x] = -1.0 - half
            coef[2 * d + 1, x] = half - 1.0
        coef[6, x] = 6.0 + diag[x]
    halo_wait(halo_w)
    once = field_stencil(w, 0)
    for x in range(bx):
        image[0, x] = once[x]
    halo_a = field_copies(1, image.at[0])
    halo_start(halo_a)
    put_row(1, once)

    zero8 = jnp.zeros((8, 2 * bz), f32)
    for p in range(area // 2):
        put_split(split0, p, jnp.concatenate(both(first_block, p) + [zero8], axis=0))
    prod = dot_nt(split0[0:96], split0[...])
    prod = prod[0:24] + prod[32:56] + prod[64:88]
    gram = prod + pltpu.roll(prod, LANES - 32, 1) + pltpu.roll(prod, LANES - 64, 1)

    row = lax.broadcasted_iota(jnp.int32, (ROWS, LANES), 0)
    lane = lax.broadcasted_iota(jnp.int32, (ROWS, LANES), 1)
    lane1 = lax.broadcasted_iota(jnp.int32, (1, LANES), 1)
    row8 = lax.broadcasted_iota(jnp.int32, (8, LANES), 0)
    lane8 = lax.broadcasted_iota(jnp.int32, (8, LANES), 1)
    row48 = lax.broadcasted_iota(jnp.int32, (2 * ROWS, LANES), 0)
    lane48 = lax.broadcasted_iota(jnp.int32, (2 * ROWS, LANES), 1)
    own8 = lane8 // UNIT == row8

    def spread(value):
        for shift in (UNIT, 2 * UNIT, 4 * UNIT):
            value = value + pltpu.roll(value, shift, 1)
        return value

    units = (
        gram[16:24],
        gram[8:16],
        jnp.where(lane8 < 8, gram[0:8], pltpu.roll(gram[16:24], LANES - 8, 1)),
    )
    packed = jnp.concatenate([
        jnp.sum(jnp.where(own8, spread(jnp.where(lane8 < UNIT, unit, 0.0)), 0.0),
                axis=0, keepdims=True)
        for unit in units], axis=0)
    gram_state = reduce_start(0, gram_buffers, packed)

    halo_wait(halo_a)
    twice_w = field_stencil(once, 1)
    for x in range(bx):
        image[1, x] = twice_w[x]
    halo_b = field_copies(2, image.at[1])
    halo_start(halo_b)
    put_row(2, twice_w)
    halo_wait(halo_r)
    rows_stencil(0, t0, t1)
    pack_faces(1, t1)
    halo_t = rows_copies(1, t1)
    halo_start(halo_t)
    for p in range(area // 2):
        put_split(split1, p, jnp.concatenate(
            both(first_block, p) + both(second_block, p), axis=0))
    prod = dot_nt(split1[...], split1[...])
    prod = prod[0:48] + prod[48:96] + prod[96:144]
    left = prod[:, 0:LANES]
    right = jnp.concatenate(
        [prod[:, LANES:], jnp.zeros((48, 2 * LANES - prod.shape[1]), f32)], axis=1)
    cross = left + pltpu.roll(left, LANES - 48, 1) + jnp.where(
        lane48 < 32, pltpu.roll(left, LANES - 96, 1), pltpu.roll(right, 32, 1))

    places = ((0, 24, 0, 24), (8, 24, 24, 24), (16, 24, 48, 24), (24, 24, 72, 24),
              (32, 32, 96, 16), (40, 40, 112, 8), (0, 22, 120, 1), (8, 22, 121, 1), (16, 22, 122, 1))
    tile = jnp.zeros((8, LANES), f32)
    for top, source, target, width in places:
        tile = jnp.where((lane8 >= target) & (lane8 < target + width),
                         pltpu.roll(cross[top:top + 8], (target - source) % LANES, 1), tile)

    gram_state = reduce_turn(0, gram_buffers, gram_state)
    back_state = reduce_start(1, back_buffers, tile)
    for x in range(bx):
        for y in range(by):
            out[pl.ds(x * by + y, ROWS, stride=area), :] = t0[x, y]
    halo_wait(halo_b)
    put_row(3, field_stencil(twice_w, 2))
    halo_wait(halo_t)
    rows_stencil(1, t1, t2)

    packed = reduce_end(gram_buffers, gram_state)
    units = [
        jnp.where(lane8 < UNIT,
                  spread(jnp.where(own8, jnp.broadcast_to(packed[u:u + 1], (8, LANES)), 0.0)),
                  0.0)
        for u in range(3)]
    corner = pltpu.roll(jnp.where(lane8 >= 8, units[2], 0.0), 8, 1)
    below = jnp.concatenate(
        [jnp.zeros((8, LANES), f32), jnp.where(lane8 < 8, units[1], 0.0), units[0],
         jnp.zeros((LANES - ROWS, LANES), f32)], axis=0)
    known = jnp.concatenate(
        [jnp.where(lane8 < 8, units[2], 0.0), units[1], units[0] + corner], axis=0)
    known = known + below.T[0:ROWS]
    known = jnp.where((lane < KEEP + 2) & (row < KEEP + 2), known, 0.0)
    norm_sq = jnp.sum(
        jnp.sum(jnp.where((lane == KEEP) & (row == KEEP), known, 0.0), axis=1, keepdims=True),
        axis=0, keepdims=True)
    scale = 1.0 / jnp.maximum(jnp.sqrt(norm_sq), 0.5)
    gram = known * jnp.where(row == KEEP, scale, 1.0) * jnp.where(lane == KEEP, scale, 1.0)
    gram = jnp.where((lane < KEEP + 1) & (row < KEEP + 1), gram, 0.0)

    def assemble(form, *extra):
        form = jnp.where(lane1 < KEEP, form, jnp.where(lane1 == KEEP, form * scale, 0.0))
        for at, value in extra:
            form = jnp.where(lane1 == at, value, form)
        return form

    def pick(form, at):
        return jnp.sum(jnp.where(lane1 == at, form, 0.0), axis=1, keepdims=True)

    def column(form, count=2 * ROWS):
        own = row48[0:count] == lane48[0:count]
        return jnp.broadcast_to(
            jnp.sum(jnp.where(own, form, 0.0), axis=1, keepdims=True), (count, LANES))

    def applied(form):
        return pltpu.roll(jnp.where(lane1 < KEEP, form, 0.0), ROWS, 1) + jnp.where(
            (lane1 == KEEP + 1) | (lane1 == KEEP + 2), pltpu.roll(form, 1, 1), 0.0)

    hcols = []

    def arnoldi(rowform, gram, count, last=False):
        c_row = jnp.where(lane1 < count, rowform, 0.0)
        twice = jnp.where(row == lane, 2.0, 0.0) - gram
        t_col = jnp.sum(twice * c_row, axis=1, keepdims=True)
        weights = jnp.broadcast_to(t_col, (ROWS, LANES))
        t_row = jnp.sum(jnp.where(row == lane, weights, 0.0), axis=0, keepdims=True)
        gt_row = jnp.sum(gram * weights, axis=0, keepdims=True)
        length_sq = jnp.sum(
            jnp.where(lane1 == ROWS - 1, rowform, t_row * (gt_row - 2.0 * c_row)),
            axis=1, keepdims=True)
        length_sq = jnp.maximum(length_sq, 0.0)
        length = jnp.sqrt(length_sq)
        inverse = 1.0 / jnp.maximum(length, 0.5)
        hcols.append(jnp.where(lane1 == count, length, t_row))
        if not last:
            e_row = t_row - c_row
            e_col = jnp.sum(jnp.where(row == lane, e_row, 0.0), axis=1, keepdims=True)
            cross_col = (e_col - jnp.sum(gram * e_row, axis=1, keepdims=True)) * inverse
            cross_row = (e_row - jnp.sum(gram * e_col, axis=0, keepdims=True)) * inverse
            corner = length_sq * inverse * inverse
            gram = jnp.where(row == count, cross_row, jnp.where(lane == count, cross_col, gram))
            gram = jnp.where((row == count) & (lane == count), corner, gram)
        return weights, t_row, inverse, gram

    image_row = known[KEEP + 1:KEEP + 2] * scale
    weights, t_row, inverse0, gram1 = arnoldi(
        assemble(image_row, (ROWS - 1, pick(image_row, KEEP + 1) * scale)), gram, KEEP + 1)
    q21 = assemble(-inverse0 * t_row, (KEEP + 1, scale * inverse0))
    a21 = applied(q21)

    turn = jnp.where(row < KEEP, weights * -inverse0, 0.0)
    chain = jnp.broadcast_to(jnp.sum(
        jnp.where(lane8 == row8 + KEEP - 5, a21, 0.0), axis=1, keepdims=True), (8, LANES))
    sums = [jnp.zeros((8, bz), f32) for _ in range(7)]
    far = []
    for x in range(bx):
        dense = jnp.zeros((by, bz), f32)
        for y in range(by):
            at = x * by + y
            v = (turn[0:8] * t2[x, y, 0:8] + turn[8:16] * t2[x, y, 8:16]
                 + (turn[16:24] * t2[x, y, 16:24] + chain * wrow[at * 8:at * 8 + 8]))
            for shift in (4, 2, 1):
                v = v + pltpu.roll(v, shift, 0)
            for k, part in enumerate(first_block(x, y) + second_block(x, y) + [v]):
                sums[k] = sums[k] + part * v
            dense = jnp.where(row3 == y, v, dense)
        far.append(dense)
    column48 = jnp.sum(jnp.concatenate(sums[0:6], axis=0), axis=1, keepdims=True)
    own = jnp.sum(jnp.where(row48 == lane48, column48, 0.0), axis=0, keepdims=True)
    own = jnp.where(lane1 == 2 * ROWS, jnp.sum(sums[6][0:1], axis=1, keepdims=True), own)
    row_state = reduce_start(2, row_buffers, own)

    back_state = reduce_turn(1, back_buffers, back_state)

    def combine(columns, x, y):
        tiles = first_block(x, y) + second_block(x, y)
        terms = [columns[8 * k:8 * k + 8] * tiles[k] for k in range(6)]
        v = (terms[0] + terms[1]) + (terms[2] + terms[3]) + (terms[4] + terms[5])
        for shift in (4, 2, 1):
            v = v + pltpu.roll(v, shift, 0)
        return v

    def field(columns, x):
        dense = jnp.zeros((by, bz), f32)
        for y in range(by):
            dense = jnp.where(row3 == y, combine(columns, x, y), dense)
        return dense

    def put_field(count, x, value):
        out[count * area + x * by:count * area + (x + 1) * by, :] = value

    q21_col = column(q21)
    for x in range(bx):
        put_field(KEEP, x, w_ref[x] * scale)
        put_field(KEEP + 1, x, field(q21_col, x))

    row_state = reduce_turn(2, row_buffers, row_state)

    tile = reduce_end(back_buffers, back_state)
    def unpack(at):
        top, source, target, width = places[at]
        return jnp.where((lane8 >= source) & (lane8 < source + width),
                         pltpu.roll(tile, (source - target) % LANES, 1), 0.0)
    square = [unpack(3 + k) for k in range(3)]
    diagonal = [jnp.where(lane8 < ROWS + 8 * (k + 1), square[k], 0.0) for k in range(3)]
    second = jnp.concatenate([unpack(6 + k) for k in range(3)], axis=0)
    over = jnp.concatenate([unpack(k) for k in range(3)], axis=0) + jnp.where(
        row < KEEP + 2, second, 0.0)
    strict = jnp.concatenate(
        [over] + [square[k] - diagonal[k] for k in range(3)]
        + [jnp.zeros((LANES - 2 * ROWS, LANES), f32)], axis=0)
    whole = jnp.concatenate(
        [known + jnp.where(row == KEEP + 2, second, 0.0)] + diagonal, axis=0)
    whole = whole + strict[0:2 * ROWS] + strict.T[0:2 * ROWS]

    def products(form_col):
        return jnp.sum(whole * form_col, axis=0, keepdims=True)

    y1 = products(column(a21))
    weights, t_row, inverse1, gram2 = arnoldi(
        assemble(y1, (KEEP + 1, jnp.sum(q21 * y1, axis=1, keepdims=True)),
                 (ROWS - 1, jnp.sum(a21 * y1, axis=1, keepdims=True))), gram1, KEEP + 2)
    t_last = pick(t_row, KEEP + 1)
    t_row = assemble(t_row)
    q22 = inverse1 * (a21 - t_row - t_last * q21)
    near = -inverse1 * (applied(t_row) + t_last * a21)
    q22_col = column(q22)
    near_col = column(near)
    y_near = products(near_col)
    for x in range(bx):
        put_field(KEEP + 2, x, field(q22_col, x))

    own = reduce_end(row_buffers, row_state)
    y2 = jnp.where(lane1 < 2 * ROWS, y_near + inverse1 * own, 0.0)
    inner = jnp.sum(jnp.concatenate([
        q21 * y2, q22 * y2,
        near * (y2 + inverse1 * own)
        + jnp.where(lane1 == 2 * ROWS, inverse1 * inverse1 * own, 0.0),
        jnp.zeros((5, LANES), f32)], axis=0), axis=1, keepdims=True)
    weights, t_row, inverse2, _ = arnoldi(
        assemble(y2, (KEEP + 1, inner[0:1]), (KEEP + 2, inner[1:2]), (ROWS - 1, inner[2:3])),
        gram2, KEEP + 3, True)
    first = jnp.where(row < KEEP, weights, jnp.where(row == KEEP, weights * scale, 0.0))
    last_col = near_col - jnp.concatenate([first, jnp.zeros((ROWS, LANES), f32)], axis=0)
    last_col = last_col - weights[KEEP + 1:KEEP + 2] * q21_col
    last_col = last_col - weights[KEEP + 2:KEEP + 3] * q22_col
    for x in range(bx):
        put_field(KEEP + 3, x, inverse2 * (field(last_col, x) + inverse1 * far[x]))

    for k in range(EXPAND):
        hess[k:k + 1] = hcols[k]
    for copies in (halo_w, halo_r, halo_a, halo_b, halo_t):
        halo_finish(copies)
    for copy in pending:
        copy.wait()


def per_device(krylov_basis, schur_vectors, next_vector, diag_shift, velocity):
    sizes = tuple(lax.axis_size(a) for a in AXES)
    block = next_vector.shape
    bx, by, bz = block
    area = bx * by
    basis = krylov_basis.shape[0]
    cells = float(area * bz * sizes[0] * sizes[1] * sizes[2])
    n0, n1 = sizes[1] * sizes[2], sizes[0]
    f32 = jnp.float32
    vmem = pl.BlockSpec(memory_space=pltpu.VMEM)
    dma = pltpu.SemaphoreType.DMA

    def buffers(rows):
        return [pltpu.VMEM((2, rows, LANES), f32), pltpu.VMEM((n0 - 1, rows, LANES), f32),
                pltpu.VMEM((n1 - 1, rows, LANES), f32)]

    vectors, columns = pl.pallas_call(
        functools.partial(body, sizes, cells),
        out_shape=(
            pltpu.VMEM((ROWS * area, bz), f32),
            pltpu.VMEM((8, LANES), f32),
        ),
        in_specs=[
            pl.BlockSpec(memory_space=pl.ANY) for _ in range(5)
        ],
        out_specs=(vmem, vmem),
        scratch_shapes=[
            pltpu.VMEM(schur_vectors.shape[::-1], f32),
            pltpu.VMEM(block, f32),
            pltpu.VMEM(block, f32),
            pltpu.VMEM((3,) + block, f32),
            pltpu.VMEM((basis * PITCH, bz), f32),
            pltpu.VMEM((7,) + block, f32),
            pltpu.VMEM((bx, by, ROWS, bz), f32),
            pltpu.VMEM((bx, by, ROWS, bz), f32),
            pltpu.VMEM((bx, by, ROWS, bz), f32),
            pltpu.VMEM((area * 8, bz), f32),
            pltpu.VMEM((2,) + block, f32),
            pltpu.VMEM((EXPAND, 2, by, bz), f32),
            pltpu.VMEM((EXPAND, 2) + block, f32),
            pltpu.VMEM((EXPAND, 2) + block, f32),
            pltpu.VMEM((2, 2, by, ROWS, bz), f32),
            pltpu.VMEM((2, 2, bx, ROWS, bz), f32),
            pltpu.VMEM((2, 2, ROWS, bz), f32),
            pltpu.VMEM((2, 2, ROWS, bz), f32),
            pltpu.VMEM((128, area * bz), jnp.bfloat16),
            pltpu.VMEM((144, area * bz), jnp.bfloat16),
            *buffers(3), *buffers(8), *buffers(1),
            dma((5,)), dma((30,)), dma((30,)), dma((6,)), dma((6,)),
        ],
        compiler_params=pltpu.CompilerParams(collective_id=0, has_side_effects=True),
    )(krylov_basis.reshape(basis, area, bz), schur_vectors.T, next_vector, diag_shift, velocity)
    return vectors.reshape((ROWS,) + block), columns[0:EXPAND, 0:ROWS].T


def solution(mesh):
    in_specs = (
        P(None, "gx", "gy", "gz"),
        P(),
        P("gx", "gy", "gz"),
        P("gx", "gy", "gz"),
        P(None, "gx", "gy", "gz"),
    )
    out_specs = (P(None, "gx", "gy", "gz"), P())
    return jax.shard_map(
        per_device, mesh=mesh, in_specs=in_specs, out_specs=out_specs, check_vma=False
    )
```

```python
import functools

import jax
import jax.numpy as jnp
from jax import lax
from jax.experimental import pallas as pl
from jax.experimental.pallas import tpu as pltpu
from jax.sharding import PartitionSpec as P

KEEP = 20
EXPAND = 3
ROWS = 24
LANES = 128
UNIT = 16
PITCH = 40
SHIFT = 4.0
AXES = ("gx", "gy", "gz")


def partner_steps(phase, sizes):
    if phase == 1:
        return [(dx, 0, 0) for dx in range(1, sizes[0])]
    return [(0, dy, dz) for dy in range(sizes[1]) for dz in range(sizes[2])][1:]


def body(
    sizes, cells,
    kry_hbm, schur_hbm, w_hbm, diag_hbm, vel_hbm,
    out, hess,
    schur, w_ref, diag, vel, kry, coef, t0, t1, t2, wrow, image,
    xs, ys, zs, xh, yh, zh, zpack, split0, split1,
    gsend, grecv0, grecv1, bsend, brecv0, brecv1, rsend, rrecv0, rrecv1,
    isend, irecv0, irecv1,
    load_sem, halo_send, halo_recv, red_send, red_recv,
):
    f32, bf16 = jnp.float32, jnp.bfloat16
    place = tuple(lax.axis_index(a) for a in AXES)
    shifted = [[lax.rem(place[d] + k, sizes[d]) for k in range(sizes[d])] for d in range(3)]

    def partners(phase):
        return [tuple(shifted[d][step[d]] for d in range(3))
                for step in partner_steps(phase, sizes)]

    barrier = pltpu.get_barrier_semaphore()
    for to in partners(0) + partners(1):
        pl.semaphore_signal(
            barrier, inc=1, device_id=to, device_id_type=pl.DeviceIdType.MESH)

    basis = kry_hbm.shape[0]
    bx, by, bz = w_ref.shape
    area = bx * by
    loads = [
        pltpu.make_async_copy(source, target, load_sem.at[k])
        for k, (source, target) in enumerate((
            (w_hbm, w_ref), (kry_hbm, kry_hbm), (schur_hbm, schur),
            (diag_hbm, diag), (vel_hbm, vel)))
    ]
    for copy in loads[:1] + loads[2:]:
        copy.start()
    for i in range(basis):
        pltpu.make_async_copy(
            kry_hbm.at[i], kry.at[pl.ds(i * PITCH, area)], load_sem.at[1]).start()
    for d, slots in enumerate(((xs, xh), (ys, yh), (zs, zh))):
        for side in (0, 1):
            def clear(slots=slots, side=side):
                for ref in slots:
                    for k in range(ref.shape[0]):
                        ref[k, side] = jnp.zeros(ref.shape[2:], f32)
            pl.when(place[d] == (0 if side == 0 else sizes[d] - 1))(clear)

    def halo_copies(kind, sources, targets):
        found = []
        for d in range(3):
            for side in (0, 1):
                at = (kind * 3 + d) * 2 + side
                to = list(place)
                to[d] = place[d] + (1 if side == 0 else -1)
                can_send = place[d] < sizes[d] - 1 if side == 0 else place[d] > 0
                can_recv = place[d] > 0 if side == 0 else place[d] < sizes[d] - 1
                found.append((
                    pltpu.make_async_remote_copy(
                        src_ref=sources[d][side], dst_ref=targets[d][side],
                        send_sem=halo_send.at[at], recv_sem=halo_recv.at[at],
                        device_id=tuple(to), device_id_type=pl.DeviceIdType.MESH,
                    ), can_send, can_recv))
        return found

    def halo_start(copies):
        for copy, can_send, _ in copies:
            pl.when(can_send)(copy.start)

    def halo_wait(copies):
        for copy, _, can_recv in copies:
            pl.when(can_recv)(copy.wait_recv)

    def halo_finish(copies):
        for copy, can_send, _ in copies:
            pl.when(can_send)(copy.wait_send)

    def field_copies(kind, ref):
        return halo_copies(
            kind,
            ((ref.at[bx - 1], ref.at[0]), (ref, ref), (ref, ref)),
            tuple((r.at[kind, 0], r.at[kind, 1]) for r in (xs, ys, zs)),
        )

    def rows_copies(level, ref):
        return halo_copies(
            EXPAND + level,
            ((ref.at[bx - 1], ref.at[0]), (ref.at[:, by - 1], ref.at[:, 0]),
             (zpack.at[level, 0], zpack.at[level, 1])),
            tuple((r.at[level, 0], r.at[level, 1]) for r in (xh, yh, zh)),
        )

    pending = []

    def exchange(kind, send, slots, phase):
        at = kind * 2 + phase
        for k, to in enumerate(partners(phase)):
            pltpu.make_async_remote_copy(
                src_ref=send, dst_ref=slots.at[k], send_sem=red_send.at[at],
                recv_sem=red_recv.at[at],
                device_id=to, device_id_type=pl.DeviceIdType.MESH,
            ).start()
        pending.append(pltpu.make_async_copy(slots, slots, red_send.at[at]))
        return pltpu.make_async_copy(slots, slots, red_recv.at[at])

    def gather_sum(arrival, own, slots):
        arrival.wait()
        terms = [own] + [slots[k] for k in range(slots.shape[0])]
        while len(terms) > 1:
            terms = [sum(terms[k + 1:k + 2], terms[k]) for k in range(0, len(terms), 2)]
        return terms[0]

    def reduce_start(kind, buffers, value):
        send, slots0, _ = buffers
        send[0] = value
        return value, exchange(kind, send.at[0], slots0, 0)

    def reduce_turn(kind, buffers, state):
        send, slots0, slots1 = buffers
        value = gather_sum(state[1], state[0], slots0)
        send[1] = value
        return value, exchange(kind, send.at[1], slots1, 1)

    def reduce_end(buffers, state):
        return gather_sum(state[1], state[0], buffers[2]) * (1.0 / cells)

    gram_buffers = (gsend, grecv0, grecv1)
    back_buffers = (bsend, brecv0, brecv1)
    row_buffers = (rsend, rrecv0, rrecv1)
    image_buffers = (isend, irecv0, irecv1)

    lane3 = lax.broadcasted_iota(jnp.int32, (by, bz), 1)
    row3 = lax.broadcasted_iota(jnp.int32, (by, bz), 0)
    lane24 = lax.broadcasted_iota(jnp.int32, (ROWS, bz), 1)

    def field_stencil(v, kind):
        res = []
        for x in range(bx):
            here = v[x]
            xb = v[x - 1] if x > 0 else xs[kind, 0]
            xa = v[x + 1] if x < bx - 1 else xs[kind, 1]
            yb = jnp.where(row3 == 0, ys[kind, 0, x, by - 1:by, :], pltpu.roll(here, 1, 0))
            ya = jnp.where(row3 == by - 1, ys[kind, 1, x, 0:1, :], pltpu.roll(here, by - 1, 0))
            zb = jnp.where(lane3 == 0, zs[kind, 0, x, :, bz - 1:bz], pltpu.roll(here, 1, 1))
            za = jnp.where(lane3 == bz - 1, zs[kind, 1, x, :, 0:1], pltpu.roll(here, bz - 1, 1))
            res.append(coef[6, x] * here + (coef[0, x] * xb + coef[1, x] * xa)
                       + (coef[2, x] * yb + coef[3, x] * ya)
                       + (coef[4, x] * zb + coef[5, x] * za))
        return res

    def rows_stencil(level, source, target):
        low, high = zh[level, 0], zh[level, 1]
        for x in range(bx):
            for y in range(by):
                at = x * by + y
                here = source[x, y]
                xb = source[x - 1, y] if x > 0 else xh[level, 0, y]
                xa = source[x + 1, y] if x < bx - 1 else xh[level, 1, y]
                yb = source[x, y - 1] if y > 0 else yh[level, 0, x]
                ya = source[x, y + 1] if y < by - 1 else yh[level, 1, x]
                zb = jnp.where(lane24 == 0, pltpu.roll(low, (bz - at) % bz, 1),
                               pltpu.roll(here, 1, 1))
                za = jnp.where(lane24 == bz - 1, pltpu.roll(high, bz - 1 - at, 1),
                               pltpu.roll(here, bz - 1, 1))
                c = [coef[k, x, y:y + 1, :] for k in range(7)]
                target[x, y] = (c[6] * here + (c[0] * xb + c[1] * xa)
                                + (c[2] * yb + c[3] * ya) + (c[4] * zb + c[5] * za))

    def pack_faces(level, source):
        for side, edge in enumerate((bz - 1, 0)):
            face = jnp.zeros((ROWS, bz), f32)
            for x in range(bx):
                for y in range(by):
                    at = x * by + y
                    face = jnp.where(
                        lane24 == at, pltpu.roll(source[x, y], (at - edge) % bz, 1), face)
            zpack[level, side] = face

    def put_row(k, tiles):
        for x in range(bx):
            wrow[pl.ds(x * by * 8 + 4 + k, by, stride=8), :] = tiles[x]

    def tail(x, y):
        return t0[x, y, 16:24] + wrow[(x * by + y) * 8:(x * by + y) * 8 + 8]

    def first_block(x, y):
        return [t0[x, y, 0:8], t0[x, y, 8:16], tail(x, y)]

    def second_block(x, y):
        return [t1[x, y, 0:8], t1[x, y, 8:16], t1[x, y, 16:24]]

    def put_split(ref, p, u):
        n = u.shape[0]
        at = pl.ds(p * 2 * bz, 2 * bz)
        high = u.astype(bf16)
        rest = u - high.astype(f32)
        mid = rest.astype(bf16)
        ref[0:n, at] = high
        ref[n:2 * n, at] = mid
        ref[2 * n:3 * n, at] = (rest - mid.astype(f32)).astype(bf16)

    def both(block, p):
        return [jnp.concatenate([block(*divmod(2 * p, by))[k], block(*divmod(2 * p + 1, by))[k]],
                                axis=1) for k in range(3)]

    dot_nt = functools.partial(
        lax.dot_general, dimension_numbers=(((1,), (1,)), ((), ())), preferred_element_type=f32)

    row = lax.broadcasted_iota(jnp.int32, (ROWS, LANES), 0)
    lane = lax.broadcasted_iota(jnp.int32, (ROWS, LANES), 1)
    lane1 = lax.broadcasted_iota(jnp.int32, (1, LANES), 1)
    row8 = lax.broadcasted_iota(jnp.int32, (8, LANES), 0)
    lane8 = lax.broadcasted_iota(jnp.int32, (8, LANES), 1)
    row48 = lax.broadcasted_iota(jnp.int32, (2 * ROWS, LANES), 0)
    lane48 = lax.broadcasted_iota(jnp.int32, (2 * ROWS, LANES), 1)

    halo_w = field_copies(0, w_ref)
    wrow[...] = jnp.zeros_like(wrow)
    t0[:, :, 16:24] = jnp.zeros((bx, by, 8, bz), f32)
    split0[96:128] = jnp.zeros((32, split0.shape[1]), bf16)
    loads[0].wait()
    pl.semaphore_wait(barrier, len(partners(0)) + len(partners(1)))
    halo_start(halo_w)
    w = [w_ref[x] for x in range(bx)]
    put_row(0, w)

    loads[2].wait()
    loads[1].wait()
    turn = schur[...]
    turn_high = turn.astype(bf16)
    turn_low = (turn - turn_high.astype(f32)).astype(bf16)
    for p in range(area // 2):
        u = jnp.concatenate([kry[pl.ds(2 * p, basis, stride=PITCH), :],
                             kry[pl.ds(2 * p + 1, basis, stride=PITCH), :]], axis=1)
        high = u.astype(bf16)
        low = (u - high.astype(f32)).astype(bf16)
        r = (jnp.dot(turn_high, high, preferred_element_type=f32)
             + (jnp.dot(turn_high, low, preferred_element_type=f32)
                + jnp.dot(turn_low, high, preferred_element_type=f32)))
        for k in (0, 1):
            x, y = divmod(2 * p + k, by)
            t0[x, y, 0:KEEP] = r[:, k * bz:(k + 1) * bz]
    pack_faces(0, t0)
    halo_r = rows_copies(0, t0)
    halo_start(halo_r)

    loads[3].wait()
    loads[4].wait()
    for x in range(bx):
        for d in range(3):
            half = 0.5 * vel[d, x]
            coef[2 * d, x] = -1.0 - half
            coef[2 * d + 1, x] = half - 1.0
        coef[6, x] = (6.0 - SHIFT) + diag[x]
    zero8 = jnp.zeros((8, 2 * bz), f32)
    for p in range(area // 2):
        put_split(split0, p, jnp.concatenate(both(first_block, p) + [zero8], axis=0))
    prod = dot_nt(split0[0:96], split0[...])
    prod = prod[0:24] + prod[32:56] + prod[64:88]
    gram = prod + pltpu.roll(prod, LANES - 32, 1) + pltpu.roll(prod, LANES - 64, 1)

    own8 = lane8 // UNIT == row8

    def spread(value):
        for shift in (UNIT, 2 * UNIT, 4 * UNIT):
            value = value + pltpu.roll(value, shift, 1)
        return value

    units = (
        gram[16:24],
        gram[8:16],
        jnp.where(lane8 < 8, gram[0:8], pltpu.roll(gram[16:24], LANES - 8, 1)),
    )
    packed = jnp.concatenate([
        jnp.sum(jnp.where(own8, spread(jnp.where(lane8 < UNIT, unit, 0.0)), 0.0),
                axis=0, keepdims=True)
        for unit in units], axis=0)
    gram_state = reduce_start(0, gram_buffers, packed)

    halo_wait(halo_w)
    once = field_stencil(w, 0)
    for x in range(bx):
        image[0, x] = once[x]
    sums = [jnp.zeros((8, bz), f32) for _ in range(3)]
    for x in range(bx):
        for y in range(by):
            v = jnp.broadcast_to(once[x][y:y + 1, :], (8, bz))
            for i, part in enumerate(first_block(x, y)):
                sums[i] = sums[i] + part * v
    squares = sum((tile * tile for tile in once[1:]), once[0] * once[0])
    column24 = jnp.sum(jnp.concatenate(sums, axis=0), axis=1, keepdims=True)
    own = jnp.sum(jnp.where(row == lane, column24, 0.0), axis=0, keepdims=True)
    own = jnp.where(lane1 == KEEP + 1, jnp.sum(
        jnp.sum(squares, axis=0, keepdims=True), axis=1, keepdims=True), own)
    image_state = reduce_start(3, image_buffers, own)
    halo_a = field_copies(1, image.at[0])
    halo_start(halo_a)
    put_row(1, once)

    halo_wait(halo_a)
    twice_w = field_stencil(once, 1)
    for x in range(bx):
        image[1, x] = twice_w[x]
    halo_b = field_copies(2, image.at[1])
    halo_start(halo_b)
    put_row(2, twice_w)
    halo_wait(halo_r)
    rows_stencil(0, t0, t1)
    pack_faces(1, t1)
    halo_t = rows_copies(1, t1)
    halo_start(halo_t)
    for p in range(area // 2):
        put_split(split1, p, jnp.concatenate(
            both(first_block, p) + both(second_block, p), axis=0))
    prod = dot_nt(split1[...], split1[...])
    prod = prod[0:48] + prod[48:96] + prod[96:144]
    left = prod[:, 0:LANES]
    right = jnp.concatenate(
        [prod[:, LANES:], jnp.zeros((48, 2 * LANES - prod.shape[1]), f32)], axis=1)
    cross = left + pltpu.roll(left, LANES - 48, 1) + jnp.where(
        lane48 < 32, pltpu.roll(left, LANES - 96, 1), pltpu.roll(right, 32, 1))

    places = ((0, 24, 0, 24), (8, 24, 24, 24), (16, 24, 48, 24), (24, 24, 72, 24),
              (32, 32, 96, 16), (40, 40, 112, 8), (0, 22, 120, 1), (8, 22, 121, 1), (16, 22, 122, 1))
    tile = jnp.zeros((8, LANES), f32)
    for top, source, target, width in places:
        tile = jnp.where((lane8 >= target) & (lane8 < target + width),
                         pltpu.roll(cross[top:top + 8], (target - source) % LANES, 1), tile)

    gram_state = reduce_turn(0, gram_buffers, gram_state)
    image_state = reduce_turn(3, image_buffers, image_state)
    back_state = reduce_start(1, back_buffers, tile)
    for x in range(bx):
        for y in range(by):
            out[pl.ds(x * by + y, ROWS, stride=area), :] = t0[x, y]
    halo_wait(halo_b)
    put_row(3, field_stencil(twice_w, 2))
    halo_wait(halo_t)
    rows_stencil(1, t1, t2)

    packed = reduce_end(gram_buffers, gram_state)
    units = [
        jnp.where(lane8 < UNIT,
                  spread(jnp.where(own8, jnp.broadcast_to(packed[u:u + 1], (8, LANES)), 0.0)),
                  0.0)
        for u in range(3)]
    corner = pltpu.roll(jnp.where(lane8 >= 8, units[2], 0.0), 8, 1)
    below = jnp.concatenate(
        [jnp.zeros((8, LANES), f32), jnp.where(lane8 < 8, units[1], 0.0), units[0],
         jnp.zeros((LANES - ROWS, LANES), f32)], axis=0)
    known = jnp.concatenate(
        [jnp.where(lane8 < 8, units[2], 0.0), units[1], units[0] + corner], axis=0)
    known = known + below.T[0:ROWS]
    known = jnp.where((lane < KEEP + 1) & (row < KEEP + 1), known, 0.0)
    norm_sq = jnp.sum(
        jnp.sum(jnp.where((lane == KEEP) & (row == KEEP), known, 0.0), axis=1, keepdims=True),
        axis=0, keepdims=True)
    scale = 1.0 / jnp.maximum(jnp.sqrt(norm_sq), 0.5)
    gram = known * jnp.where(row == KEEP, scale, 1.0) * jnp.where(lane == KEEP, scale, 1.0)
    shifted_row = SHIFT * known[KEEP:KEEP + 1]

    def assemble(form, *extra):
        form = jnp.where(lane1 < KEEP, form, jnp.where(lane1 == KEEP, form * scale, 0.0))
        for at, value in extra:
            form = jnp.where(lane1 == at, value, form)
        return form

    def pick(form, at):
        return jnp.sum(jnp.where(lane1 == at, form, 0.0), axis=1, keepdims=True)

    def column(form, count=2 * ROWS):
        own = row48[0:count] == lane48[0:count]
        return jnp.broadcast_to(
            jnp.sum(jnp.where(own, form, 0.0), axis=1, keepdims=True), (count, LANES))

    def applied(form):
        return pltpu.roll(jnp.where(lane1 < KEEP, form, 0.0), ROWS, 1) + jnp.where(
            (lane1 == KEEP + 1) | (lane1 == KEEP + 2), pltpu.roll(form, 1, 1), 0.0)

    hcols = []

    def arnoldi(rowform, gram, count, last=False):
        c_row = jnp.where(lane1 < count, rowform, 0.0)
        twice = jnp.where(row == lane, 2.0, 0.0) - gram
        t_col = jnp.sum(twice * c_row, axis=1, keepdims=True)
        weights = jnp.broadcast_to(t_col, (ROWS, LANES))
        t_row = jnp.sum(jnp.where(row == lane, weights, 0.0), axis=0, keepdims=True)
        gt_row = jnp.sum(gram * weights, axis=0, keepdims=True)
        length_sq = jnp.sum(
            jnp.where(lane1 == ROWS - 1, rowform, t_row * (gt_row - 2.0 * c_row)),
            axis=1, keepdims=True)
        length_sq = jnp.maximum(length_sq, 0.0)
        length = jnp.sqrt(length_sq)
        inverse = 1.0 / jnp.maximum(length, 0.5)
        hcols.append(jnp.where(lane1 == count, length, t_row))
        if not last:
            e_row = t_row - c_row
            e_col = jnp.sum(jnp.where(row == lane, e_row, 0.0), axis=1, keepdims=True)
            cross_col = (e_col - jnp.sum(gram * e_row, axis=1, keepdims=True)) * inverse
            cross_row = (e_row - jnp.sum(gram * e_col, axis=0, keepdims=True)) * inverse
            corner = length_sq * inverse * inverse
            gram = jnp.where(row == count, cross_row, jnp.where(lane == count, cross_col, gram))
            gram = jnp.where((row == count) & (lane == count), corner, gram)
        return weights, t_row, inverse, gram

    known_row = reduce_end(image_buffers, image_state)
    image_sq = jnp.sum(jnp.where(lane1 == KEEP + 1, known_row, jnp.where(
        lane1 == KEEP, SHIFT * (2.0 * known_row + shifted_row), 0.0)),
        axis=1, keepdims=True) * (scale * scale)
    image_row = (known_row + shifted_row) * scale
    weights, t_row, inverse0, gram1 = arnoldi(
        assemble(image_row, (ROWS - 1, image_sq)), gram, KEEP + 1)
    q21 = assemble(-inverse0 * t_row, (KEEP + 1, scale * inverse0)) + jnp.where(
        lane1 == KEEP, SHIFT * scale * inverse0, 0.0)
    b21 = applied(q21)
    a21 = b21 + SHIFT * q21

    turn = jnp.where(row < KEEP, -weights, 0.0)
    chain = jnp.where(row8 == 6, (SHIFT - weights[KEEP:KEEP + 1]) * scale,
                      jnp.where(row8 == 7, scale, 0.0))
    sums = [jnp.zeros((8, bz), f32) for _ in range(7)]
    far = []
    for x in range(bx):
        dense = jnp.zeros((by, bz), f32)
        for y in range(by):
            at = x * by + y
            v = (turn[0:8] * t2[x, y, 0:8] + turn[8:16] * t2[x, y, 8:16]
                 + (turn[16:24] * t2[x, y, 16:24] + chain * wrow[at * 8:at * 8 + 8]))
            for shift in (4, 2, 1):
                v = v + pltpu.roll(v, shift, 0)
            for k, part in enumerate(first_block(x, y) + second_block(x, y) + [v]):
                sums[k] = sums[k] + part * v
            dense = jnp.where(row3 == y, v, dense)
        far.append(dense)
    column48 = jnp.sum(jnp.concatenate(sums[0:6], axis=0), axis=1, keepdims=True)
    own = jnp.sum(jnp.where(row48 == lane48, column48, 0.0), axis=0, keepdims=True)
    own = jnp.where(lane1 == 2 * ROWS, jnp.sum(sums[6][0:1], axis=1, keepdims=True) * inverse0, own)
    own = own * inverse0
    row_state = reduce_start(2, row_buffers, own)

    back_state = reduce_turn(1, back_buffers, back_state)

    def combine(columns, x, y):
        tiles = first_block(x, y) + second_block(x, y)
        terms = [columns[8 * k:8 * k + 8] * tiles[k] for k in range(6)]
        v = (terms[0] + terms[1]) + (terms[2] + terms[3]) + (terms[4] + terms[5])
        for shift in (4, 2, 1):
            v = v + pltpu.roll(v, shift, 0)
        return v

    def field(columns, x):
        dense = jnp.zeros((by, bz), f32)
        for y in range(by):
            dense = jnp.where(row3 == y, combine(columns, x, y), dense)
        return dense

    def put_field(count, x, value):
        out[count * area + x * by:count * area + (x + 1) * by, :] = value

    q21_col = column(q21)
    for x in range(bx):
        put_field(KEEP, x, w_ref[x] * scale)
        put_field(KEEP + 1, x, field(q21_col, x))

    row_state = reduce_turn(2, row_buffers, row_state)

    tile = reduce_end(back_buffers, back_state)
    def unpack(at):
        top, source, target, width = places[at]
        return jnp.where((lane8 >= source) & (lane8 < source + width),
                         pltpu.roll(tile, (source - target) % LANES, 1), 0.0)
    square = [unpack(3 + k) for k in range(3)]
    diagonal = [jnp.where(lane8 < ROWS + 8 * (k + 1), square[k], 0.0) for k in range(3)]
    second = jnp.concatenate([unpack(6 + k) for k in range(3)], axis=0)
    over = jnp.concatenate([unpack(k) for k in range(3)], axis=0) + jnp.where(
        row < KEEP + 2, second, 0.0)
    strict = jnp.concatenate(
        [over] + [square[k] - diagonal[k] for k in range(3)]
        + [jnp.zeros((LANES - 2 * ROWS, LANES), f32)], axis=0)
    known_col = column(known_row, ROWS)
    known = jnp.where(row == KEEP + 1, jnp.where(lane < KEEP + 2, known_row, 0.0),
                      jnp.where((lane == KEEP + 1) & (row < KEEP + 1), known_col, known))
    whole = jnp.concatenate(
        [known + jnp.where(row == KEEP + 2, second, 0.0)] + diagonal, axis=0)
    whole = whole + strict[0:2 * ROWS] + strict.T[0:2 * ROWS]

    def products(form_col):
        return jnp.sum(whole * form_col, axis=0, keepdims=True)

    y1 = products(column(a21))
    weights, t_row, inverse1, gram2 = arnoldi(
        assemble(y1, (KEEP + 1, jnp.sum(q21 * y1, axis=1, keepdims=True)),
                 (ROWS - 1, jnp.sum(a21 * y1, axis=1, keepdims=True))), gram1, KEEP + 2)
    t_last = pick(t_row, KEEP + 1)
    t_row = assemble(t_row)
    q22 = inverse1 * (a21 - t_row - t_last * q21)
    near = inverse1 * ((SHIFT - t_last) * b21 - applied(t_row)) + SHIFT * q22
    q22_col = column(q22)
    near_col = column(near)
    y_near = products(near_col)
    for x in range(bx):
        put_field(KEEP + 2, x, field(q22_col, x))

    own = reduce_end(row_buffers, row_state)
    y2 = jnp.where(lane1 < 2 * ROWS, y_near + inverse1 * own, 0.0)
    inner = jnp.sum(jnp.concatenate([
        q21 * y2, q22 * y2,
        near * (y2 + inverse1 * own)
        + jnp.where(lane1 == 2 * ROWS, inverse1 * inverse1 * own, 0.0),
        jnp.zeros((5, LANES), f32)], axis=0), axis=1, keepdims=True)
    weights, t_row, inverse2, _ = arnoldi(
        assemble(y2, (KEEP + 1, inner[0:1]), (KEEP + 2, inner[1:2]), (ROWS - 1, inner[2:3])),
        gram2, KEEP + 3, True)
    first = jnp.where(row < KEEP, weights, jnp.where(row == KEEP, weights * scale, 0.0))
    last_col = near_col - jnp.concatenate([first, jnp.zeros((ROWS, LANES), f32)], axis=0)
    last_col = last_col - weights[KEEP + 1:KEEP + 2] * q21_col
    last_col = last_col - weights[KEEP + 2:KEEP + 3] * q22_col
    for x in range(bx):
        put_field(KEEP + 3, x, inverse2 * (field(last_col, x) + inverse1 * inverse0 * far[x]))

    for k in range(EXPAND):
        hess[k:k + 1] = hcols[k]
    for copies in (halo_w, halo_r, halo_a, halo_b, halo_t):
        halo_finish(copies)
    for copy in pending:
        copy.wait()


def place_results(vectors, columns, out, hess, small, sem):
    large = pltpu.make_async_copy(vectors, out, sem.at[0])
    large.start()
    small[...] = columns[0:EXPAND, 0:ROWS]
    copy = pltpu.make_async_copy(small, hess, sem.at[1])
    copy.start()
    copy.wait()
    large.wait()


def per_device(krylov_basis, schur_vectors, next_vector, diag_shift, velocity):
    sizes = tuple(lax.axis_size(a) for a in AXES)
    block = next_vector.shape
    bx, by, bz = block
    area = bx * by
    basis = krylov_basis.shape[0]
    cells = float(area * bz * sizes[0] * sizes[1] * sizes[2])
    n0, n1 = sizes[1] * sizes[2], sizes[0]
    f32 = jnp.float32
    vmem = pl.BlockSpec(memory_space=pltpu.VMEM)
    dma = pltpu.SemaphoreType.DMA

    def buffers(rows):
        return [pltpu.VMEM((2, rows, LANES), f32), pltpu.VMEM((n0 - 1, rows, LANES), f32),
                pltpu.VMEM((n1 - 1, rows, LANES), f32)]

    vectors, columns = pl.pallas_call(
        functools.partial(body, sizes, cells),
        out_shape=(
            pltpu.VMEM((ROWS * area, bz), f32),
            pltpu.VMEM((8, LANES), f32),
        ),
        in_specs=[
            pl.BlockSpec(memory_space=pl.ANY) for _ in range(5)
        ],
        out_specs=(vmem, vmem),
        scratch_shapes=[
            pltpu.VMEM(schur_vectors.shape[::-1], f32),
            pltpu.VMEM(block, f32),
            pltpu.VMEM(block, f32),
            pltpu.VMEM((3,) + block, f32),
            pltpu.VMEM((basis * PITCH, bz), f32),
            pltpu.VMEM((7,) + block, f32),
            pltpu.VMEM((bx, by, ROWS, bz), f32),
            pltpu.VMEM((bx, by, ROWS, bz), f32),
            pltpu.VMEM((bx, by, ROWS, bz), f32),
            pltpu.VMEM((area * 8, bz), f32),
            pltpu.VMEM((2,) + block, f32),
            pltpu.VMEM((EXPAND, 2, by, bz), f32),
            pltpu.VMEM((EXPAND, 2) + block, f32),
            pltpu.VMEM((EXPAND, 2) + block, f32),
            pltpu.VMEM((2, 2, by, ROWS, bz), f32),
            pltpu.VMEM((2, 2, bx, ROWS, bz), f32),
            pltpu.VMEM((2, 2, ROWS, bz), f32),
            pltpu.VMEM((2, 2, ROWS, bz), f32),
            pltpu.VMEM((128, area * bz), jnp.bfloat16),
            pltpu.VMEM((144, area * bz), jnp.bfloat16),
            *buffers(3), *buffers(8), *buffers(1), *buffers(1),
            dma((5,)), dma((30,)), dma((30,)), dma((8,)), dma((8,)),
        ],
        compiler_params=pltpu.CompilerParams(collective_id=0, has_side_effects=True),
    )(krylov_basis.reshape(basis, area, bz), schur_vectors.T, next_vector, diag_shift, velocity)
    whole = pl.BlockSpec(memory_space=pl.ANY)
    vectors, columns = pl.pallas_call(
        place_results,
        out_shape=(
            jax.ShapeDtypeStruct((ROWS * area, bz), f32),
            jax.ShapeDtypeStruct((EXPAND, ROWS), f32),
        ),
        in_specs=[vmem, vmem],
        out_specs=(whole, whole),
        scratch_shapes=[pltpu.VMEM((EXPAND, ROWS), f32), dma((2,))],
    )(*(pltpu.with_memory_space_constraint(a, pltpu.VMEM) for a in (vectors, columns)))
    return vectors.reshape((ROWS,) + block), columns.T


def solution(mesh):
    in_specs = (
        P(None, "gx", "gy", "gz"),
        P(),
        P("gx", "gy", "gz"),
        P("gx", "gy", "gz"),
        P(None, "gx", "gy", "gz"),
    )
    out_specs = (P(None, "gx", "gy", "gz"), P())
    return jax.shard_map(
        per_device, mesh=mesh, in_specs=in_specs, out_specs=out_specs, check_vma=False
    )
```

```python
import functools

import jax
import jax.numpy as jnp
from jax import lax
from jax.experimental import pallas as pl
from jax.experimental.pallas import tpu as pltpu
from jax.sharding import PartitionSpec as P

KEEP = 20
EXPAND = 3
ROWS = 24
LANES = 128
UNIT = 16
PITCH = 40
SHIFT = 4.0
AXES = ("gx", "gy", "gz")


def partner_steps(phase, sizes):
    if phase == 1:
        steps = [(dx, 0, 0) for dx in range(1, sizes[0])]
    else:
        steps = [(0, dy, dz) for dy in range(sizes[1]) for dz in range(sizes[2])][1:]
    return sorted(steps, key=lambda step: -sum(
        min(step[d], sizes[d] - step[d]) for d in range(3)))


def body(
    sizes, cells,
    kry_hbm, schur_hbm, w_hbm, diag_hbm, vel_hbm,
    out, hess,
    schur, w_ref, diag, vel, kry, coef, t0, t1, t2, wrow, image,
    xs, ys, zs, zsend, xh, yh, zh, zpack, split0, split1, split2,
    gsend, grecv0, grecv1, bsend, brecv0, brecv1, isend, irecv0, irecv1,
    psend, precv, csend, crecv, rsend, rrecv,
    load_sem, halo_send, halo_recv, red_send, red_recv,
):
    f32, bf16 = jnp.float32, jnp.bfloat16
    place = tuple(lax.axis_index(a) for a in AXES)
    shifted = [[lax.rem(place[d] + k, sizes[d]) for k in range(sizes[d])] for d in range(3)]

    def partners(phase):
        return [tuple(shifted[d][step[d]] for d in range(3))
                for step in partner_steps(phase, sizes)]

    barrier = pltpu.get_barrier_semaphore()
    for to in partners(0) + partners(1):
        pl.semaphore_signal(
            barrier, inc=1, device_id=to, device_id_type=pl.DeviceIdType.MESH)

    basis = kry_hbm.shape[0]
    bx, by, bz = w_ref.shape
    area = bx * by
    loads = [
        pltpu.make_async_copy(source, target, load_sem.at[k])
        for k, (source, target) in enumerate((
            (w_hbm, w_ref), (kry_hbm, kry_hbm), (schur_hbm, schur),
            (diag_hbm, diag), (vel_hbm, vel)))
    ]
    for copy in loads[:1] + loads[2:]:
        copy.start()
    for i in range(basis):
        pltpu.make_async_copy(
            kry_hbm.at[i], kry.at[pl.ds(i * PITCH, area)], load_sem.at[1]).start()
    for d, slots in enumerate(((xs, xh), (ys, yh), (zs, zh))):
        for side in (0, 1):
            def clear(slots=slots, side=side):
                for ref in slots:
                    for k in range(ref.shape[0]):
                        ref[k, side] = jnp.zeros(ref.shape[2:], f32)
            pl.when(place[d] == (0 if side == 0 else sizes[d] - 1))(clear)

    def halo_copies(kind, sources, targets):
        found = []
        for d in range(3):
            for side in (0, 1):
                at = (kind * 3 + d) * 2 + side
                to = list(place)
                to[d] = place[d] + (1 if side == 0 else -1)
                can_send = place[d] < sizes[d] - 1 if side == 0 else place[d] > 0
                can_recv = place[d] > 0 if side == 0 else place[d] < sizes[d] - 1
                found.append((
                    pltpu.make_async_remote_copy(
                        src_ref=sources[d][side], dst_ref=targets[d][side],
                        send_sem=halo_send.at[at], recv_sem=halo_recv.at[at],
                        device_id=tuple(to), device_id_type=pl.DeviceIdType.MESH,
                    ), can_send, can_recv))
        return found

    def halo_start(copies):
        for copy, can_send, _ in copies:
            pl.when(can_send)(copy.start)

    def halo_wait(copies):
        for copy, _, can_recv in copies:
            pl.when(can_recv)(copy.wait_recv)

    def halo_finish(copies):
        for copy, can_send, _ in copies:
            pl.when(can_send)(copy.wait_send)

    def field_copies(kind, ref):
        return halo_copies(
            kind,
            ((ref.at[bx - 1], ref.at[0]), (ref.at[:, by - 1:by], ref.at[:, 0:1]),
             (zsend.at[kind, 0], zsend.at[kind, 1])),
            tuple((r.at[kind, 0], r.at[kind, 1]) for r in (xs, ys, zs)),
        )

    def rows_copies(level, ref):
        return halo_copies(
            EXPAND + level,
            ((ref.at[bx - 1], ref.at[0]), (ref.at[:, by - 1], ref.at[:, 0]),
             (zpack.at[level, 0], zpack.at[level, 1])),
            tuple((r.at[level, 0], r.at[level, 1]) for r in (xh, yh, zh)),
        )

    pending = []

    def exchange(kind, send, slots, phase):
        at = kind * 2 + phase
        for k, to in enumerate(partners(phase)):
            pltpu.make_async_remote_copy(
                src_ref=send, dst_ref=slots.at[k], send_sem=red_send.at[at],
                recv_sem=red_recv.at[at],
                device_id=to, device_id_type=pl.DeviceIdType.MESH,
            ).start()
        pending.append(pltpu.make_async_copy(slots, slots, red_send.at[at]))
        return pltpu.make_async_copy(slots, slots, red_recv.at[at])

    def gather_sum(arrival, own, slots):
        arrival.wait()
        terms = [own] + [slots[k] for k in range(slots.shape[0])]
        while len(terms) > 1:
            terms = [sum(terms[k + 1:k + 2], terms[k]) for k in range(0, len(terms), 2)]
        return terms[0]

    def reduce_start(kind, buffers, value):
        send, slots0, _ = buffers
        send[0] = value
        return value, exchange(kind, send.at[0], slots0, 0)

    def reduce_turn(kind, buffers, state):
        send, slots0, slots1 = buffers
        value = gather_sum(state[1], state[0], slots0)
        send[1] = value
        return value, exchange(kind, send.at[1], slots1, 1)

    def reduce_end(buffers, state):
        return gather_sum(state[1], state[0], buffers[2]) * (1.0 / cells)

    gram_buffers = (gsend, grecv0, grecv1)
    back_buffers = (bsend, brecv0, brecv1)
    image_buffers = (isend, irecv0, irecv1)

    lane3 = lax.broadcasted_iota(jnp.int32, (by, bz), 1)
    row3 = lax.broadcasted_iota(jnp.int32, (by, bz), 0)
    lane24 = lax.broadcasted_iota(jnp.int32, (ROWS, bz), 1)

    def field_stencil(v, kind):
        res = []
        for x in range(bx):
            here = v[x]
            xb = v[x - 1] if x > 0 else xs[kind, 0]
            xa = v[x + 1] if x < bx - 1 else xs[kind, 1]
            yb = jnp.where(row3 == 0, ys[kind, 0, x], pltpu.roll(here, 1, 0))
            ya = jnp.where(row3 == by - 1, ys[kind, 1, x], pltpu.roll(here, by - 1, 0))
            zb = jnp.where(lane3 == 0, zs[kind, 0, :, x:x + 1], pltpu.roll(here, 1, 1))
            za = jnp.where(lane3 == bz - 1, zs[kind, 1, :, x:x + 1], pltpu.roll(here, bz - 1, 1))
            res.append(coef[6, x] * here + (coef[0, x] * xb + coef[1, x] * xa)
                       + (coef[2, x] * yb + coef[3, x] * ya)
                       + (coef[4, x] * zb + coef[5, x] * za))
        return res

    def rows_stencil(level, source, target):
        low, high = zh[level, 0], zh[level, 1]
        for x in range(bx):
            for y in range(by):
                at = x * by + y
                here = source[x, y]
                xb = source[x - 1, y] if x > 0 else xh[level, 0, y]
                xa = source[x + 1, y] if x < bx - 1 else xh[level, 1, y]
                yb = source[x, y - 1] if y > 0 else yh[level, 0, x]
                ya = source[x, y + 1] if y < by - 1 else yh[level, 1, x]
                zb = jnp.where(lane24 == 0, pltpu.roll(low, (bz - at) % bz, 1),
                               pltpu.roll(here, 1, 1))
                za = jnp.where(lane24 == bz - 1, pltpu.roll(high, bz - 1 - at, 1),
                               pltpu.roll(here, bz - 1, 1))
                c = [coef[k, x, y:y + 1, :] for k in range(7)]
                target[x, y] = (c[6] * here + (c[0] * xb + c[1] * xa)
                                + (c[2] * yb + c[3] * ya) + (c[4] * zb + c[5] * za))

    def pack_ends(kind, tiles):
        for side, edge in enumerate((bz - 1, 0)):
            face = tiles[0] if edge == 0 else pltpu.roll(tiles[0], 1, 1)
            for x in range(1, bx):
                face = jnp.where(lane3 == x, pltpu.roll(tiles[x], (x - edge) % bz, 1), face)
            zsend[kind, side] = face

    def pack_faces(level, source):
        for side, edge in enumerate((bz - 1, 0)):
            face = jnp.zeros((ROWS, bz), f32)
            for x in range(bx):
                for y in range(by):
                    at = x * by + y
                    face = jnp.where(
                        lane24 == at, pltpu.roll(source[x, y], (at - edge) % bz, 1), face)
            zpack[level, side] = face

    def put_row(k, tiles):
        for x in range(bx):
            wrow[pl.ds(x * by * 8 + 4 + k, by, stride=8), :] = tiles[x]

    def tail(x, y):
        return t0[x, y, 16:24] + wrow[(x * by + y) * 8:(x * by + y) * 8 + 8]

    def first_block(x, y):
        return [t0[x, y, 0:8], t0[x, y, 8:16], tail(x, y)]

    def second_block(x, y):
        return [t1[x, y, 0:8], t1[x, y, 8:16], t1[x, y, 16:24]]

    def third_block(x, y):
        return [t2[x, y, 0:8], t2[x, y, 8:16], t2[x, y, 16:24]]

    def row_dots(tiles, *blocks):
        sums = [jnp.zeros((8, bz), f32) for _ in range(3 * len(blocks))]
        for x in range(bx):
            for y in range(by):
                v = jnp.broadcast_to(tiles[x][y:y + 1, :], (8, bz))
                for k, part in enumerate([t for block in blocks for t in block(x, y)]):
                    sums[k] = sums[k] + part * v
        return [jnp.sum(total, axis=1, keepdims=True) for total in sums]

    def as_row(columns):
        count = 8 * len(columns)
        own = (lax.broadcasted_iota(jnp.int32, (count, LANES), 0)
               == lax.broadcasted_iota(jnp.int32, (count, LANES), 1))
        return jnp.sum(jnp.where(own, jnp.concatenate(columns, axis=0), 0.0), axis=0, keepdims=True)

    def put_split(ref, p, u, first=0, pitch=None):
        n = u.shape[0]
        pitch = pitch or n
        at = pl.ds(p * 2 * bz, 2 * bz)
        high = u.astype(bf16)
        rest = u - high.astype(f32)
        mid = rest.astype(bf16)
        ref[first:first + n, at] = high
        ref[first + pitch:first + pitch + n, at] = mid
        ref[first + 2 * pitch:first + 2 * pitch + n, at] = (rest - mid.astype(f32)).astype(bf16)

    def both(block, p):
        return [jnp.concatenate([block(*divmod(2 * p, by))[k], block(*divmod(2 * p + 1, by))[k]],
                                axis=1) for k in range(3)]

    dot_nt = functools.partial(
        lax.dot_general, dimension_numbers=(((1,), (1,)), ((), ())), preferred_element_type=f32)

    row = lax.broadcasted_iota(jnp.int32, (ROWS, LANES), 0)
    lane = lax.broadcasted_iota(jnp.int32, (ROWS, LANES), 1)
    lane1 = lax.broadcasted_iota(jnp.int32, (1, LANES), 1)
    row8 = lax.broadcasted_iota(jnp.int32, (8, LANES), 0)
    lane8 = lax.broadcasted_iota(jnp.int32, (8, LANES), 1)
    row48 = lax.broadcasted_iota(jnp.int32, (2 * ROWS, LANES), 0)
    lane48 = lax.broadcasted_iota(jnp.int32, (2 * ROWS, LANES), 1)

    halo_w = field_copies(0, w_ref)
    wrow[...] = jnp.zeros_like(wrow)
    t0[:, :, 16:24] = jnp.zeros((bx, by, 8, bz), f32)
    split0[96:128] = jnp.zeros((32, split0.shape[1]), bf16)
    split2[96:128] = jnp.zeros((32, split2.shape[1]), bf16)

    loads[2].wait()
    loads[1].wait()
    turn = schur[...]
    turn_high = turn.astype(bf16)
    turn_low = (turn - turn_high.astype(f32)).astype(bf16)
    for p in range(area // 2):
        u = jnp.concatenate([kry[pl.ds(2 * p, basis, stride=PITCH), :],
                             kry[pl.ds(2 * p + 1, basis, stride=PITCH), :]], axis=1)
        high = u.astype(bf16)
        low = (u - high.astype(f32)).astype(bf16)
        r = (jnp.dot(turn_high, high, preferred_element_type=f32)
             + (jnp.dot(turn_high, low, preferred_element_type=f32)
                + jnp.dot(turn_low, high, preferred_element_type=f32)))
        for k in (0, 1):
            x, y = divmod(2 * p + k, by)
            t0[x, y, 0:KEEP] = r[:, k * bz:(k + 1) * bz]
    pack_faces(0, t0)
    halo_r = rows_copies(0, t0)
    loads[0].wait()
    w = [w_ref[x] for x in range(bx)]
    pack_ends(0, w)
    put_row(0, w)
    pl.semaphore_wait(barrier, len(partners(0)) + len(partners(1)))
    halo_start(halo_w)
    halo_start(halo_r)

    loads[3].wait()
    loads[4].wait()
    for x in range(bx):
        for d in range(3):
            half = 0.5 * vel[d, x]
            coef[2 * d, x] = -1.0 - half
            coef[2 * d + 1, x] = half - 1.0
        coef[6, x] = (6.0 - SHIFT) + diag[x]
    zero8 = jnp.zeros((8, 2 * bz), f32)
    for p in range(area // 2):
        put_split(split0, p, jnp.concatenate(both(first_block, p) + [zero8], axis=0))
    prod = dot_nt(split0[0:96], split0[...])
    prod = prod[0:24] + prod[32:56] + prod[64:88]
    gram = prod + pltpu.roll(prod, LANES - 32, 1) + pltpu.roll(prod, LANES - 64, 1)

    own8 = lane8 // UNIT == row8

    def spread(value):
        for shift in (UNIT, 2 * UNIT, 4 * UNIT):
            value = value + pltpu.roll(value, shift, 1)
        return value

    units = (
        gram[16:24],
        gram[8:16],
        jnp.where(lane8 < 8, gram[0:8], pltpu.roll(gram[16:24], LANES - 8, 1)),
    )
    packed = jnp.concatenate([
        jnp.sum(jnp.where(own8, spread(jnp.where(lane8 < UNIT, unit, 0.0)), 0.0),
                axis=0, keepdims=True)
        for unit in units], axis=0)
    gram_state = reduce_start(0, gram_buffers, packed)

    halo_wait(halo_w)
    once = field_stencil(w, 0)
    for x in range(bx):
        image[0, x] = once[x]
    pack_ends(1, once)
    own = as_row(row_dots(once, first_block))
    squares = sum((tile * tile for tile in once[1:]), once[0] * once[0])
    own = jnp.where(lane1 == KEEP + 1, jnp.sum(
        jnp.sum(squares, axis=0, keepdims=True), axis=1, keepdims=True), own)
    image_state = reduce_start(3, image_buffers, own)
    halo_a = field_copies(1, image.at[0])
    halo_start(halo_a)
    put_row(1, once)

    halo_wait(halo_r)
    rows_stencil(0, t0, t1)
    pack_faces(1, t1)
    halo_t = rows_copies(1, t1)
    halo_start(halo_t)
    for p in range(area // 2):
        put_split(split1, p, jnp.concatenate(
            both(first_block, p) + both(second_block, p), axis=0))
    prod = dot_nt(split1[...], split1[...])
    prod = prod[0:48] + prod[48:96] + prod[96:144]
    left = prod[:, 0:LANES]
    right = jnp.concatenate(
        [prod[:, LANES:], jnp.zeros((48, 2 * LANES - prod.shape[1]), f32)], axis=1)
    cross = left + pltpu.roll(left, LANES - 48, 1) + jnp.where(
        lane48 < 32, pltpu.roll(left, LANES - 96, 1), pltpu.roll(right, 32, 1))

    halo_wait(halo_a)
    twice_w = field_stencil(once, 1)
    for x in range(bx):
        image[1, x] = twice_w[x]
    pack_ends(2, twice_w)
    halo_b = field_copies(2, image.at[1])
    halo_start(halo_b)
    put_row(2, twice_w)

    places = ((0, 24, 0, 24), (8, 24, 24, 24), (16, 24, 48, 24), (24, 24, 72, 24),
              (32, 32, 96, 16), (40, 40, 112, 8))
    tile = jnp.zeros((8, LANES), f32)
    for top, source, target, width in places:
        tile = jnp.where((lane8 >= target) & (lane8 < target + width),
                         pltpu.roll(cross[top:top + 8], (target - source) % LANES, 1), tile)
    for k, col in enumerate(row_dots(twice_w, first_block, second_block)):
        tile = jnp.where(lane8 == 120 + k, col, tile)
    back_state = reduce_start(1, back_buffers, tile)
    for p in range(area // 2):
        put_split(split1, p, jnp.concatenate(
            both(first_block, p)[2:3] + both(second_block, p)[0:1], axis=0), 16, 2 * ROWS)

    halo_wait(halo_t)
    rows_stencil(1, t1, t2)
    def third_tail(x, y):
        return third_block(x, y)[0:2] + [t2[x, y, 16:24]
                                         + wrow[(x * by + y) * 8:(x * by + y) * 8 + 8]]
    for p in range(area // 2):
        put_split(split2, p, jnp.concatenate(both(third_tail, p) + [zero8], axis=0))

    def fold(prod):
        return prod + pltpu.roll(prod, LANES - 32, 1) + pltpu.roll(prod, LANES - 64, 1)

    prod = dot_nt(split1[...], split2[...])
    mixed = fold(prod[0:48] + prod[48:96] + prod[96:144])
    prod = dot_nt(split2[0:96], split2[...])
    square = fold(prod[0:24] + prod[32:56] + prod[64:88])

    def pack_mixed(value):
        tile = jnp.zeros((8, LANES), f32)
        for k in range(5):
            tile = jnp.where((lane8 >= ROWS * k) & (lane8 < ROWS * k + ROWS),
                             pltpu.roll(value[8 * k:8 * k + 8], ROWS * k, 1), tile)
        return tile

    def pack_square(last, value):
        tile = jnp.where(lane8 < ROWS, last, 0.0)
        start = ROWS
        for k in range(3):
            width = ROWS - 8 * k
            for half in (0, 1):
                part = value[8 * k:8 * k + 8]
                if half:
                    part = pltpu.roll(part, 4, 0)
                tile = jnp.where((lane8 >= start) & (lane8 < start + width),
                                 pltpu.roll(part, (start - 8 * k) % LANES, 1), tile)
                start = start + width
        return tile

    gram_state = reduce_turn(0, gram_buffers, gram_state)
    image_state = reduce_turn(3, image_buffers, image_state)
    tile = pack_mixed(mixed)
    psend[0] = tile[0:4]
    psend[1] = tile[4:8]
    psend[2] = pack_square(mixed[40:48], square)[0:4]
    mixed_arrival = exchange(2, psend, precv, 1)

    halo_wait(halo_b)
    thrice_w = field_stencil(twice_w, 2)
    put_row(3, thrice_w)
    csend[...] = as_row(row_dots(thrice_w, first_block, second_block, third_block))
    chain_arrival = exchange(4, csend, crecv, 1)
    for x in range(bx):
        for y in range(by):
            out[pl.ds(x * by + y, ROWS, stride=area), :] = t0[x, y]
    back_state = reduce_turn(1, back_buffers, back_state)

    packed = reduce_end(gram_buffers, gram_state)
    units = [
        jnp.where(lane8 < UNIT,
                  spread(jnp.where(own8, jnp.broadcast_to(packed[u:u + 1], (8, LANES)), 0.0)),
                  0.0)
        for u in range(3)]
    corner = pltpu.roll(jnp.where(lane8 >= 8, units[2], 0.0), 8, 1)
    below = jnp.concatenate(
        [jnp.zeros((8, LANES), f32), jnp.where(lane8 < 8, units[1], 0.0), units[0],
         jnp.zeros((LANES - ROWS, LANES), f32)], axis=0)
    known = jnp.concatenate(
        [jnp.where(lane8 < 8, units[2], 0.0), units[1], units[0] + corner], axis=0)
    known = known + below.T[0:ROWS]
    known = jnp.where((lane < KEEP + 1) & (row < KEEP + 1), known, 0.0)
    norm_sq = jnp.sum(
        jnp.sum(jnp.where((lane == KEEP) & (row == KEEP), known, 0.0), axis=1, keepdims=True),
        axis=0, keepdims=True)
    scale = 1.0 / jnp.maximum(jnp.sqrt(norm_sq), 0.5)
    gram = known * jnp.where(row == KEEP, scale, 1.0) * jnp.where(lane == KEEP, scale, 1.0)
    shifted_row = SHIFT * known[KEEP:KEEP + 1]

    def assemble(form, *extra):
        form = jnp.where(lane1 < KEEP, form, jnp.where(lane1 == KEEP, form * scale, 0.0))
        for at, value in extra:
            form = jnp.where(lane1 == at, value, form)
        return form

    def pick(form, at):
        return jnp.sum(jnp.where(lane1 == at, form, 0.0), axis=1, keepdims=True)

    def column(form, count=2 * ROWS):
        own = row48[0:count] == lane48[0:count]
        return jnp.broadcast_to(
            jnp.sum(jnp.where(own, form, 0.0), axis=1, keepdims=True), (count, LANES))

    def applied(form):
        return pltpu.roll(jnp.where(lane1 < KEEP, form, 0.0), ROWS, 1) + jnp.where(
            (lane1 == KEEP + 1) | (lane1 == KEEP + 2), pltpu.roll(form, 1, 1), 0.0)

    hcols = []

    def arnoldi(rowform, gram, count, last=False):
        c_row = jnp.where(lane1 < count, rowform, 0.0)
        twice = jnp.where(row == lane, 2.0, 0.0) - gram
        t_col = jnp.sum(twice * c_row, axis=1, keepdims=True)
        weights = jnp.broadcast_to(t_col, (ROWS, LANES))
        t_row = jnp.sum(jnp.where(row == lane, weights, 0.0), axis=0, keepdims=True)
        gt_row = jnp.sum(gram * weights, axis=0, keepdims=True)
        length_sq = jnp.sum(
            jnp.where(lane1 == ROWS - 1, rowform, t_row * (gt_row - 2.0 * c_row)),
            axis=1, keepdims=True)
        length_sq = jnp.maximum(length_sq, 0.0)
        length = jnp.sqrt(length_sq)
        inverse = 1.0 / jnp.maximum(length, 0.5)
        hcols.append(jnp.where(lane1 == count, length, t_row))
        if not last:
            e_row = t_row - c_row
            e_col = jnp.sum(jnp.where(row == lane, e_row, 0.0), axis=1, keepdims=True)
            cross_col = (e_col - jnp.sum(gram * e_row, axis=1, keepdims=True)) * inverse
            cross_row = (e_row - jnp.sum(gram * e_col, axis=0, keepdims=True)) * inverse
            corner = length_sq * inverse * inverse
            gram = jnp.where(row == count, cross_row, jnp.where(lane == count, cross_col, gram))
            gram = jnp.where((row == count) & (lane == count), corner, gram)
        return weights, t_row, inverse, gram

    known_row = reduce_end(image_buffers, image_state)
    image_sq = jnp.sum(jnp.where(lane1 == KEEP + 1, known_row, jnp.where(
        lane1 == KEEP, SHIFT * (2.0 * known_row + shifted_row), 0.0)),
        axis=1, keepdims=True) * (scale * scale)
    image_row = (known_row + shifted_row) * scale
    weights, t_row, inverse0, gram1 = arnoldi(
        assemble(image_row, (ROWS - 1, image_sq)), gram, KEEP + 1)
    q21 = assemble(-inverse0 * t_row, (KEEP + 1, scale * inverse0)) + jnp.where(
        lane1 == KEEP, SHIFT * scale * inverse0, 0.0)
    b21 = applied(q21)
    a21 = b21 + SHIFT * q21

    q_square = jnp.where(lane1 < KEEP, q21, 0.0) + jnp.where(
        lane1 == KEEP + 2, pltpu.roll(q21, 2, 1), 0.0)
    q_last = pick(q21, KEEP + 1)
    spread_q = jnp.broadcast_to(q_square, (2 * ROWS, LANES))
    pairs = column(q_square, ROWS) * q_square * jnp.where(lane < row // 8 * 8 + 8, 1.0, 2.0)
    weigh_mixed = pack_mixed(spread_q)
    weigh_square = pack_square(spread_q[0:8], pairs)[0:4]
    weigh_chain = q_last * (2.0 * pltpu.roll(jnp.where(lane1 < KEEP, q21, 0.0), 2 * ROWS, 1)
                            + jnp.where(lane1 == KEEP + 2, 2.0 * q_square, 0.0)
                            + jnp.where(lane1 == KEEP + 3, q_last, 0.0))
    chain_row = gather_sum(chain_arrival, csend[...], crecv)
    chain_sq = jnp.sum(chain_row * weigh_chain, axis=1, keepdims=True)
    total = gather_sum(mixed_arrival, psend[...], precv)
    tile = jnp.concatenate([total[0], total[1]], axis=0) * weigh_mixed
    last = total[2] * weigh_square
    lane4 = lax.broadcasted_iota(jnp.int32, (4, LANES), 1)
    columns = [jnp.sum(jnp.where((lane8 >= ROWS * k) & (lane8 < ROWS * k + ROWS), tile, 0.0),
                       axis=1, keepdims=True) for k in range(5)]
    columns.append(jnp.concatenate([
        jnp.sum(jnp.where(lane4 < ROWS, last, 0.0), axis=1, keepdims=True),
        jnp.zeros((4, 1), f32)], axis=0))
    far_sq = chain_sq + jnp.sum(jnp.sum(
        jnp.where(lane4 < ROWS, 0.0, last), axis=0, keepdims=True), axis=1, keepdims=True)
    own = jnp.where(lane1 < 2 * ROWS, as_row(columns) + q_last * chain_row, 0.0)
    own = jnp.where(lane1 == 2 * ROWS, far_sq, own)
    rsend[...] = own
    row_state = own, exchange(2, rsend, rrecv, 0)

    turn = jnp.where(row < KEEP, -weights, 0.0)
    chain = jnp.where(row8 == 6, (SHIFT - weights[KEEP:KEEP + 1]) * scale,
                      jnp.where(row8 == 7, scale, 0.0))
    far = []
    for x in range(bx):
        dense = jnp.zeros((by, bz), f32)
        for y in range(by):
            at = x * by + y
            v = (turn[0:8] * t2[x, y, 0:8] + turn[8:16] * t2[x, y, 8:16]
                 + (turn[16:24] * t2[x, y, 16:24] + chain * wrow[at * 8:at * 8 + 8]))
            for shift in (4, 2, 1):
                v = v + pltpu.roll(v, shift, 0)
            dense = jnp.where(row3 == y, v, dense)
        far.append(dense)

    def combine(columns, x, y):
        tiles = first_block(x, y) + second_block(x, y)
        terms = [columns[8 * k:8 * k + 8] * tiles[k] for k in range(6)]
        v = (terms[0] + terms[1]) + (terms[2] + terms[3]) + (terms[4] + terms[5])
        for shift in (4, 2, 1):
            v = v + pltpu.roll(v, shift, 0)
        return v

    def field(columns, x):
        dense = jnp.zeros((by, bz), f32)
        for y in range(by):
            dense = jnp.where(row3 == y, combine(columns, x, y), dense)
        return dense

    def put_field(count, x, value):
        out[count * area + x * by:count * area + (x + 1) * by, :] = value

    q21_col = column(q21)
    for x in range(bx):
        put_field(KEEP, x, w_ref[x] * scale)
        put_field(KEEP + 1, x, field(q21_col, x))

    tile = reduce_end(back_buffers, back_state)
    def unpack(at):
        top, source, target, width = places[at]
        return jnp.where((lane8 >= source) & (lane8 < source + width),
                         pltpu.roll(tile, (source - target) % LANES, 1), 0.0)
    square = [unpack(3 + k) for k in range(3)]
    diagonal = [jnp.where(lane8 < ROWS + 8 * (k + 1), square[k], 0.0) for k in range(3)]
    columns = [jnp.where(lane8 == KEEP + 2, pltpu.roll(tile, (KEEP + 2 - 120 - k) % LANES, 1), 0.0)
               for k in range(6)]
    second = jnp.concatenate(columns[0:3], axis=0)
    over = jnp.concatenate([unpack(k) for k in range(3)], axis=0) + jnp.where(
        row < KEEP + 2, second, 0.0)
    strict = jnp.concatenate(
        [over] + [square[k] - diagonal[k] + columns[3 + k] for k in range(3)]
        + [jnp.zeros((LANES - 2 * ROWS, LANES), f32)], axis=0)
    known_col = column(known_row, ROWS)
    known = jnp.where(row == KEEP + 1, jnp.where(lane < KEEP + 2, known_row, 0.0),
                      jnp.where((lane == KEEP + 1) & (row < KEEP + 1), known_col, known))
    whole = jnp.concatenate(
        [known + jnp.where(row == KEEP + 2, second, 0.0)] + diagonal, axis=0)
    whole = whole + strict[0:2 * ROWS] + strict.T[0:2 * ROWS]

    def products(form_col):
        return jnp.sum(whole * form_col, axis=0, keepdims=True)

    y1 = products(column(a21))
    weights, t_row, inverse1, gram2 = arnoldi(
        assemble(y1, (KEEP + 1, jnp.sum(q21 * y1, axis=1, keepdims=True)),
                 (ROWS - 1, jnp.sum(a21 * y1, axis=1, keepdims=True))), gram1, KEEP + 2)
    t_last = pick(t_row, KEEP + 1)
    t_row = assemble(t_row)
    q22 = inverse1 * (a21 - t_row - t_last * q21)
    near = inverse1 * ((SHIFT - t_last) * b21 - applied(t_row)) + SHIFT * q22
    q22_col = column(q22)
    near_col = column(near)
    y_near = products(near_col)
    for x in range(bx):
        put_field(KEEP + 2, x, field(q22_col, x))

    for copies in (halo_w, halo_r, halo_a, halo_b, halo_t):
        halo_finish(copies)
    for copy in pending[:-1]:
        copy.wait()

    own = gather_sum(row_state[1], row_state[0], rrecv) * (1.0 / cells)
    y2 = jnp.where(lane1 < 2 * ROWS, y_near + inverse1 * own, 0.0)
    inner = jnp.sum(jnp.concatenate([
        q21 * y2, q22 * y2,
        near * (y2 + inverse1 * own)
        + jnp.where(lane1 == 2 * ROWS, inverse1 * inverse1 * own, 0.0),
        jnp.zeros((5, LANES), f32)], axis=0), axis=1, keepdims=True)
    weights, t_row, inverse2, _ = arnoldi(
        assemble(y2, (KEEP + 1, inner[0:1]), (KEEP + 2, inner[1:2]), (ROWS - 1, inner[2:3])),
        gram2, KEEP + 3, True)
    first = jnp.where(row < KEEP, weights, jnp.where(row == KEEP, weights * scale, 0.0))
    last_col = near_col - jnp.concatenate([first, jnp.zeros((ROWS, LANES), f32)], axis=0)
    last_col = last_col - weights[KEEP + 1:KEEP + 2] * q21_col
    last_col = last_col - weights[KEEP + 2:KEEP + 3] * q22_col
    for x in range(bx):
        put_field(KEEP + 3, x, inverse2 * (field(last_col, x) + inverse1 * inverse0 * far[x]))

    for k in range(EXPAND):
        hess[k:k + 1] = hcols[k]
    pending[-1].wait()


def place_results(vectors, columns, out, hess, small, sem):
    large = pltpu.make_async_copy(vectors, out, sem.at[0])
    large.start()
    small[...] = columns[0:EXPAND, 0:ROWS]
    copy = pltpu.make_async_copy(small, hess, sem.at[1])
    copy.start()
    copy.wait()
    large.wait()


def per_device(krylov_basis, schur_vectors, next_vector, diag_shift, velocity):
    sizes = tuple(lax.axis_size(a) for a in AXES)
    block = next_vector.shape
    bx, by, bz = block
    area = bx * by
    basis = krylov_basis.shape[0]
    cells = float(area * bz * sizes[0] * sizes[1] * sizes[2])
    n0, n1 = sizes[1] * sizes[2], sizes[0]
    f32 = jnp.float32
    vmem = pl.BlockSpec(memory_space=pltpu.VMEM)
    dma = pltpu.SemaphoreType.DMA

    def buffers(rows):
        return [pltpu.VMEM((2, rows, LANES), f32), pltpu.VMEM((n0 - 1, rows, LANES), f32),
                pltpu.VMEM((n1 - 1, rows, LANES), f32)]

    vectors, columns = pl.pallas_call(
        functools.partial(body, sizes, cells),
        out_shape=(
            pltpu.VMEM((ROWS * area, bz), f32),
            pltpu.VMEM((8, LANES), f32),
        ),
        in_specs=[
            pl.BlockSpec(memory_space=pl.ANY) for _ in range(5)
        ],
        out_specs=(vmem, vmem),
        scratch_shapes=[
            pltpu.VMEM(schur_vectors.shape[::-1], f32),
            pltpu.VMEM(block, f32),
            pltpu.VMEM(block, f32),
            pltpu.VMEM((3,) + block, f32),
            pltpu.VMEM((basis * PITCH, bz), f32),
            pltpu.VMEM((7,) + block, f32),
            pltpu.VMEM((bx, by, ROWS, bz), f32),
            pltpu.VMEM((bx, by, ROWS, bz), f32),
            pltpu.VMEM((bx, by, ROWS, bz), f32),
            pltpu.VMEM((area * 8, bz), f32),
            pltpu.VMEM((2,) + block, f32),
            pltpu.VMEM((EXPAND, 2, by, bz), f32),
            pltpu.VMEM((EXPAND, 2, bx, 1, bz), f32),
            pltpu.VMEM((EXPAND, 2, by, bz), f32),
            pltpu.VMEM((EXPAND, 2, by, bz), f32),
            pltpu.VMEM((2, 2, by, ROWS, bz), f32),
            pltpu.VMEM((2, 2, bx, ROWS, bz), f32),
            pltpu.VMEM((2, 2, ROWS, bz), f32),
            pltpu.VMEM((2, 2, ROWS, bz), f32),
            pltpu.VMEM((128, area * bz), jnp.bfloat16),
            pltpu.VMEM((144, area * bz), jnp.bfloat16),
            pltpu.VMEM((128, area * bz), jnp.bfloat16),
            *buffers(3), *buffers(8), *buffers(1),
            pltpu.VMEM((3, 4, LANES), f32), pltpu.VMEM((n1 - 1, 3, 4, LANES), f32),
            pltpu.VMEM((1, LANES), f32), pltpu.VMEM((n1 - 1, 1, LANES), f32),
            pltpu.VMEM((1, LANES), f32), pltpu.VMEM((n0 - 1, 1, LANES), f32),
            dma((5,)), dma((30,)), dma((30,)), dma((10,)), dma((10,)),
        ],
        compiler_params=pltpu.CompilerParams(collective_id=0, has_side_effects=True),
    )(krylov_basis.reshape(basis, area, bz), schur_vectors.T, next_vector, diag_shift, velocity)
    whole = pl.BlockSpec(memory_space=pl.ANY)
    vectors, columns = pl.pallas_call(
        place_results,
        out_shape=(
            jax.ShapeDtypeStruct((ROWS * area, bz), f32),
            jax.ShapeDtypeStruct((EXPAND, ROWS), f32),
        ),
        in_specs=[vmem, vmem],
        out_specs=(whole, whole),
        scratch_shapes=[pltpu.VMEM((EXPAND, ROWS), f32), dma((2,))],
    )(*(pltpu.with_memory_space_constraint(a, pltpu.VMEM) for a in (vectors, columns)))
    return vectors.reshape((ROWS,) + block), columns.T


def solution(mesh):
    in_specs = (
        P(None, "gx", "gy", "gz"),
        P(),
        P("gx", "gy", "gz"),
        P("gx", "gy", "gz"),
        P(None, "gx", "gy", "gz"),
    )
    out_specs = (P(None, "gx", "gy", "gz"), P())
    return jax.shard_map(
        per_device, mesh=mesh, in_specs=in_specs, out_specs=out_specs, check_vma=False
    )
```

```python
import functools

import jax
import jax.numpy as jnp
from jax import lax
from jax.experimental import pallas as pl
from jax.experimental.pallas import tpu as pltpu
from jax.sharding import PartitionSpec as P

KEEP = 20
EXPAND = 3
ROWS = 24
LANES = 128
UNIT = 16
PITCH = 40
SHIFT = 4.0
AXES = ("gx", "gy", "gz")


def partner_steps(phase, sizes):
    if phase == 1:
        steps = [(dx, 0, 0) for dx in range(1, sizes[0])]
    else:
        steps = [(0, dy, dz) for dy in range(sizes[1]) for dz in range(sizes[2])][1:]
    return sorted(steps, key=lambda step: -sum(
        min(step[d], sizes[d] - step[d]) for d in range(3)))


def body(
    sizes, cells,
    kry_hbm, schur_hbm, w_hbm, diag_hbm, vel_hbm,
    out, hess,
    schur, w_ref, diag, vel, kry, coef, t0, t1, t2, wrow, image,
    hw, hr, faces, zpack, split0, split1, split2,
    gsend, gslots, bsend, bslots, psend, precv, isend, csend, rsend, rslots,
    load_sem, halo_send, halo_recv, red_send, red_recv,
):
    f32, bf16 = jnp.float32, jnp.bfloat16
    place = tuple(lax.axis_index(a) for a in AXES)
    shifted = [[lax.rem(place[d] + k, sizes[d]) for k in range(sizes[d])] for d in range(3)]

    def partners(phase):
        return [tuple(shifted[d][step[d]] for d in range(3))
                for step in partner_steps(phase, sizes)]

    barrier = pltpu.get_barrier_semaphore()
    for to in partners(0) + partners(1):
        pl.semaphore_signal(
            barrier, inc=1, device_id=to, device_id_type=pl.DeviceIdType.MESH)

    basis = kry_hbm.shape[0]
    bx, by, bz = w_ref.shape
    area = bx * by
    loads = [
        pltpu.make_async_copy(source, target, load_sem.at[k])
        for k, (source, target) in enumerate((
            (w_hbm, w_ref), (kry_hbm, kry_hbm), (schur_hbm, schur),
            (diag_hbm, diag), (vel_hbm, vel)))
    ]
    for copy in loads[:1] + loads[2:]:
        copy.start()
    for i in range(basis):
        pltpu.make_async_copy(
            kry_hbm.at[i], kry.at[pl.ds(i * PITCH, area)], load_sem.at[1]).start()
    def halo_copies(sources, targets, send, recv):
        found = []
        for d in range(3):
            for side in (0, 1):
                to = list(place)
                to[d] = shifted[d][1 if side == 0 else sizes[d] - 1]
                found.append(pltpu.make_async_remote_copy(
                    src_ref=sources[d][side], dst_ref=targets[d][side],
                    send_sem=halo_send.at[send], recv_sem=halo_recv.at[recv],
                    device_id=tuple(to), device_id_type=pl.DeviceIdType.MESH,
                ))
        return found

    def halo_start(copies):
        for copy in copies:
            copy.start()

    def field_wait(kind):
        pltpu.make_async_copy(hw.at[kind], hw.at[kind], halo_recv.at[kind]).wait()

    def rows_wait(level):
        landed = hr.at[level, :, :, 0:KEEP]
        pltpu.make_async_copy(landed, landed, halo_recv.at[EXPAND + level]).wait()

    def field_copies(kind, ref):
        return halo_copies(
            ((ref.at[bx - 1], ref.at[0]), (faces.at[kind, 0, 0], faces.at[kind, 1, 0]),
             (faces.at[kind, 0, 1], faces.at[kind, 1, 1])),
            tuple((hw.at[kind, 0, d], hw.at[kind, 1, d]) for d in range(3)), 0, kind)

    def rows_copies(level, ref):
        return halo_copies(
            ((ref.at[bx - 1, :, 0:KEEP], ref.at[0, :, 0:KEEP]),
             (ref.at[:, by - 1, 0:KEEP], ref.at[:, 0, 0:KEEP]),
             (zpack.at[level, 0, 0:KEEP], zpack.at[level, 1, 0:KEEP])),
            tuple((hr.at[level, 0, part, 0:KEEP], hr.at[level, 1, part, 0:KEEP])
                  for part in (pl.ds(0, by), pl.ds(by, bx), by + bx)), 1, EXPAND + level)

    def exchange(kind, at, send, slots, phase):
        for k, to in enumerate(partners(phase)):
            pltpu.make_async_remote_copy(
                src_ref=send, dst_ref=slots.at[k], send_sem=red_send.at[kind],
                recv_sem=red_recv.at[at],
                device_id=to, device_id_type=pl.DeviceIdType.MESH,
            ).start()
        return pltpu.make_async_copy(slots, slots, red_recv.at[at])

    def gather_sum(arrival, own, slots):
        arrival.wait()
        terms = [own] + [slots[k] for k in range(slots.shape[0])]
        while len(terms) > 1:
            terms = [sum(terms[k + 1:k + 2], terms[k]) for k in range(0, len(terms), 2)]
        return terms[0]

    def reduce_start(buffers, value):
        kind, at, send, slots0, _ = buffers
        send[0] = value
        return value, exchange(kind, at, send.at[0], slots0, 0)

    def reduce_turn(buffers, state):
        kind, at, send, slots0, slots1 = buffers
        value = gather_sum(state[1], state[0], slots0)
        send[1] = value
        return value, exchange(kind, at + 1, send.at[1], slots1, 1)

    def reduce_end(buffers, state):
        return gather_sum(state[1], state[0], buffers[4]) * (1.0 / cells)

    n0, n1 = len(partner_steps(0, sizes)), len(partner_steps(1, sizes))
    gram_buffers = (0, 0, gsend, gslots.at[pl.ds(0, n0)], gslots.at[pl.ds(n0, n1)])
    back_buffers = (1, 2, bsend, bslots.at[pl.ds(0, n0)], bslots.at[pl.ds(n0, n1)])
    image_buffers = (3, 4, isend, rslots.at[pl.ds(0, n0)], rslots.at[pl.ds(n0, n1)])
    crecv = rslots.at[pl.ds(n0 + n1, n1)]
    rrecv = rslots.at[pl.ds(n0 + 2 * n1, n0)]

    lane3 = lax.broadcasted_iota(jnp.int32, (by, bz), 1)
    row3 = lax.broadcasted_iota(jnp.int32, (by, bz), 0)
    lane24 = lax.broadcasted_iota(jnp.int32, (ROWS, bz), 1)

    def field_stencil(v, kind):
        res = []
        for x in range(bx):
            here = v[x]
            xb = v[x - 1] if x > 0 else hw[kind, 0, 0]
            xa = v[x + 1] if x < bx - 1 else hw[kind, 1, 0]
            yb = jnp.where(row3 == 0, hw[kind, 0, 1, x:x + 1, :], pltpu.roll(here, 1, 0))
            ya = jnp.where(row3 == by - 1, hw[kind, 1, 1, x:x + 1, :], pltpu.roll(here, by - 1, 0))
            zb = jnp.where(lane3 == 0, hw[kind, 0, 2, :, x:x + 1], pltpu.roll(here, 1, 1))
            za = jnp.where(lane3 == bz - 1, hw[kind, 1, 2, :, x:x + 1], pltpu.roll(here, bz - 1, 1))
            res.append(coef[6, x] * here + (coef[0, x] * xb + coef[1, x] * xa)
                       + (coef[2, x] * yb + coef[3, x] * ya)
                       + (coef[4, x] * zb + coef[5, x] * za))
        return res

    inner = [(x, y) for x in range(1, bx - 1) for y in range(1, by - 1)]
    outer = [(x, y) for x in range(bx) for y in range(by) if (x, y) not in inner]

    def rows_stencil(level, source, target, where):
        low, high = hr[level, 0, by + bx], hr[level, 1, by + bx]
        for x, y in where:
            at = x * by + y
            here = source[x, y]
            xb = source[x - 1, y] if x > 0 else hr[level, 0, y]
            xa = source[x + 1, y] if x < bx - 1 else hr[level, 1, y]
            yb = source[x, y - 1] if y > 0 else hr[level, 0, by + x]
            ya = source[x, y + 1] if y < by - 1 else hr[level, 1, by + x]
            zb = jnp.where(lane24 == 0, pltpu.roll(low, (bz - at) % bz, 1),
                           pltpu.roll(here, 1, 1))
            za = jnp.where(lane24 == bz - 1, pltpu.roll(high, bz - 1 - at, 1),
                           pltpu.roll(here, bz - 1, 1))
            c = [coef[k, x, y:y + 1, :] for k in range(7)]
            target[x, y] = (c[6] * here + (c[0] * xb + c[1] * xa)
                            + (c[2] * yb + c[3] * ya) + (c[4] * zb + c[5] * za))

    def pack_ends(kind, tiles):
        for side, (near, edge) in enumerate(((by - 1, bz - 1), (0, 0))):
            rows = jnp.zeros((by, bz), f32)
            lanes = jnp.zeros((by, bz), f32)
            for x in range(bx):
                rows = jnp.where(row3 == x, pltpu.roll(tiles[x], (x - near) % by, 0), rows)
                lanes = jnp.where(lane3 == x, pltpu.roll(tiles[x], (x - edge) % bz, 1), lanes)
            faces[kind, side, 0] = rows
            faces[kind, side, 1] = lanes

    def pack_faces(level, source):
        for side, edge in enumerate((bz - 1, 0)):
            face = jnp.zeros((ROWS, bz), f32)
            for x in range(bx):
                for y in range(by):
                    at = x * by + y
                    face = jnp.where(
                        lane24 == at, pltpu.roll(source[x, y], (at - edge) % bz, 1), face)
            zpack[level, side] = face

    def put_row(k, tiles):
        for x in range(bx):
            wrow[pl.ds(x * by * 8 + 4 + k, by, stride=8), :] = tiles[x]

    def tail(x, y):
        return t0[x, y, 16:24] + wrow[(x * by + y) * 8:(x * by + y) * 8 + 8]

    def first_block(x, y):
        return [t0[x, y, 0:8], t0[x, y, 8:16], tail(x, y)]

    def second_block(x, y):
        return [t1[x, y, 0:8], t1[x, y, 8:16], t1[x, y, 16:24]]

    def third_block(x, y):
        return [t2[x, y, 0:8], t2[x, y, 8:16], t2[x, y, 16:24]]

    def row_dots(tiles, *blocks):
        sums = [jnp.zeros((8, bz), f32) for _ in range(3 * len(blocks))]
        for x in range(bx):
            for y in range(by):
                v = jnp.broadcast_to(tiles[x][y:y + 1, :], (8, bz))
                for k, part in enumerate([t for block in blocks for t in block(x, y)]):
                    sums[k] = sums[k] + part * v
        return [jnp.sum(total, axis=1, keepdims=True) for total in sums]

    def as_row(columns):
        count = 8 * len(columns)
        own = (lax.broadcasted_iota(jnp.int32, (count, LANES), 0)
               == lax.broadcasted_iota(jnp.int32, (count, LANES), 1))
        return jnp.sum(jnp.where(own, jnp.concatenate(columns, axis=0), 0.0), axis=0, keepdims=True)

    def put_split(ref, p, u, first=0, pitch=None):
        n = u.shape[0]
        pitch = pitch or n
        at = pl.ds(p * 2 * bz, 2 * bz)
        high = u.astype(bf16)
        rest = u - high.astype(f32)
        mid = rest.astype(bf16)
        ref[first:first + n, at] = high
        ref[first + pitch:first + pitch + n, at] = mid
        ref[first + 2 * pitch:first + 2 * pitch + n, at] = (rest - mid.astype(f32)).astype(bf16)

    def both(block, p):
        return [jnp.concatenate([block(*divmod(2 * p, by))[k], block(*divmod(2 * p + 1, by))[k]],
                                axis=1) for k in range(3)]

    dot_nt = functools.partial(
        lax.dot_general, dimension_numbers=(((1,), (1,)), ((), ())), preferred_element_type=f32)

    row = lax.broadcasted_iota(jnp.int32, (ROWS, LANES), 0)
    lane = lax.broadcasted_iota(jnp.int32, (ROWS, LANES), 1)
    lane1 = lax.broadcasted_iota(jnp.int32, (1, LANES), 1)
    row8 = lax.broadcasted_iota(jnp.int32, (8, LANES), 0)
    lane8 = lax.broadcasted_iota(jnp.int32, (8, LANES), 1)
    row48 = lax.broadcasted_iota(jnp.int32, (2 * ROWS, LANES), 0)
    lane48 = lax.broadcasted_iota(jnp.int32, (2 * ROWS, LANES), 1)

    halo_w = field_copies(0, w_ref)
    wrow[...] = jnp.zeros_like(wrow)
    hr[:, :, :, KEEP:ROWS] = jnp.zeros(hr.shape[0:3] + (ROWS - KEEP, bz), f32)
    t0[:, :, 16:24] = jnp.zeros((bx, by, 8, bz), f32)
    split0[96:128] = jnp.zeros((32, split0.shape[1]), bf16)
    split2[96:128] = jnp.zeros((32, split2.shape[1]), bf16)

    loads[2].wait()
    loads[1].wait()
    turn = schur[...]
    turn_high = turn.astype(bf16)
    turn_low = (turn - turn_high.astype(f32)).astype(bf16)
    for p in range(area // 2):
        u = jnp.concatenate([kry[pl.ds(2 * p, basis, stride=PITCH), :],
                             kry[pl.ds(2 * p + 1, basis, stride=PITCH), :]], axis=1)
        high = u.astype(bf16)
        low = (u - high.astype(f32)).astype(bf16)
        r = (jnp.dot(turn_high, high, preferred_element_type=f32)
             + (jnp.dot(turn_high, low, preferred_element_type=f32)
                + jnp.dot(turn_low, high, preferred_element_type=f32)))
        for k in (0, 1):
            x, y = divmod(2 * p + k, by)
            t0[x, y, 0:KEEP] = r[:, k * bz:(k + 1) * bz]
    pack_faces(0, t0)
    halo_r = rows_copies(0, t0)
    loads[0].wait()
    w = [w_ref[x] for x in range(bx)]
    pack_ends(0, w)
    put_row(0, w)
    pl.semaphore_wait(barrier, len(partners(0)) + len(partners(1)))
    halo_start(halo_w)
    halo_start(halo_r)

    loads[3].wait()
    loads[4].wait()
    for x in range(bx):
        for d in range(3):
            half = 0.5 * vel[d, x]
            at = (x, row3, lane3)[d]
            span = (bx, by, bz)[d]
            coef[2 * d, x] = jnp.where((at == 0) & (place[d] == 0), 0.0, -1.0 - half)
            coef[2 * d + 1, x] = jnp.where(
                (at == span - 1) & (place[d] == sizes[d] - 1), 0.0, half - 1.0)
        coef[6, x] = (6.0 - SHIFT) + diag[x]
    zero8 = jnp.zeros((8, 2 * bz), f32)
    for p in range(area // 2):
        put_split(split0, p, jnp.concatenate(both(first_block, p) + [zero8], axis=0))
    prod = dot_nt(split0[0:96], split0[...])
    prod = prod[0:24] + prod[32:56] + prod[64:88]
    gram = prod + pltpu.roll(prod, LANES - 32, 1) + pltpu.roll(prod, LANES - 64, 1)

    own8 = lane8 // UNIT == row8

    def spread(value):
        for shift in (UNIT, 2 * UNIT, 4 * UNIT):
            value = value + pltpu.roll(value, shift, 1)
        return value

    units = (
        gram[16:24],
        gram[8:16],
        jnp.where(lane8 < 8, gram[0:8], pltpu.roll(gram[16:24], LANES - 8, 1)),
    )
    packed = jnp.concatenate([
        jnp.sum(jnp.where(own8, spread(jnp.where(lane8 < UNIT, unit, 0.0)), 0.0),
                axis=0, keepdims=True)
        for unit in units], axis=0)
    gram_state = reduce_start(gram_buffers, packed)

    field_wait(0)
    once = field_stencil(w, 0)
    for x in range(bx):
        image[0, x] = once[x]
    pack_ends(1, once)
    halo_a = field_copies(1, image.at[0])
    halo_start(halo_a)
    own = as_row(row_dots(once, first_block))
    squares = sum((tile * tile for tile in once[1:]), once[0] * once[0])
    own = jnp.where(lane1 == KEEP + 1, jnp.sum(
        jnp.sum(squares, axis=0, keepdims=True), axis=1, keepdims=True), own)
    image_state = reduce_start(image_buffers, own)
    put_row(1, once)

    rows_wait(0)
    halo_t = rows_copies(1, t1)
    rows_stencil(0, t0, t1, outer)
    halo_start(halo_t[0:4])
    rows_stencil(0, t0, t1, inner)
    pack_faces(1, t1)
    halo_start(halo_t[4:6])
    for p in range(area // 2):
        put_split(split1, p, jnp.concatenate(
            both(first_block, p) + both(second_block, p), axis=0))
    prod = dot_nt(split1[...], split1[...])
    prod = prod[0:48] + prod[48:96] + prod[96:144]
    left = prod[:, 0:LANES]
    right = jnp.concatenate(
        [prod[:, LANES:], jnp.zeros((48, 2 * LANES - prod.shape[1]), f32)], axis=1)
    cross = left + pltpu.roll(left, LANES - 48, 1) + jnp.where(
        lane48 < 32, pltpu.roll(left, LANES - 96, 1), pltpu.roll(right, 32, 1))

    field_wait(1)
    twice_w = field_stencil(once, 1)
    for x in range(bx):
        image[1, x] = twice_w[x]
    pack_ends(2, twice_w)
    halo_b = field_copies(2, image.at[1])
    halo_start(halo_b)
    put_row(2, twice_w)

    places = ((0, 24, 0, 24), (8, 24, 24, 24), (16, 24, 48, 24), (24, 24, 72, 24),
              (32, 32, 96, 16), (40, 40, 112, 8))
    tile = jnp.zeros((8, LANES), f32)
    for top, source, target, width in places:
        tile = jnp.where((lane8 >= target) & (lane8 < target + width),
                         pltpu.roll(cross[top:top + 8], (target - source) % LANES, 1), tile)
    for k, col in enumerate(row_dots(twice_w, first_block, second_block)):
        tile = jnp.where(lane8 == 120 + k, col, tile)
    back_state = reduce_start(back_buffers, tile)
    for p in range(area // 2):
        put_split(split1, p, jnp.concatenate(
            both(first_block, p)[2:3] + both(second_block, p)[0:1], axis=0), 16, 2 * ROWS)

    rows_wait(1)
    rows_stencil(1, t1, t2, outer + inner)
    def third_tail(x, y):
        return third_block(x, y)[0:2] + [t2[x, y, 16:24]
                                         + wrow[(x * by + y) * 8:(x * by + y) * 8 + 8]]
    for p in range(area // 2):
        put_split(split2, p, jnp.concatenate(both(third_tail, p) + [zero8], axis=0))

    def fold(prod):
        return prod + pltpu.roll(prod, LANES - 32, 1) + pltpu.roll(prod, LANES - 64, 1)

    prod = dot_nt(split1[...], split2[...])
    mixed = fold(prod[0:48] + prod[48:96] + prod[96:144])
    prod = dot_nt(split2[0:96], split2[...])
    square = fold(prod[0:24] + prod[32:56] + prod[64:88])

    def pack_mixed(value):
        tile = jnp.zeros((8, LANES), f32)
        for k in range(5):
            tile = jnp.where((lane8 >= ROWS * k) & (lane8 < ROWS * k + ROWS),
                             pltpu.roll(value[8 * k:8 * k + 8], ROWS * k, 1), tile)
        return tile

    def pack_square(last, value):
        tile = jnp.where(lane8 < ROWS, last, 0.0)
        start = ROWS
        for k in range(3):
            width = ROWS - 8 * k
            for half in (0, 1):
                part = value[8 * k:8 * k + 8]
                if half:
                    part = pltpu.roll(part, 4, 0)
                tile = jnp.where((lane8 >= start) & (lane8 < start + width),
                                 pltpu.roll(part, (start - 8 * k) % LANES, 1), tile)
                start = start + width
        return tile

    gram_state = reduce_turn(gram_buffers, gram_state)
    image_state = reduce_turn(image_buffers, image_state)
    tile = pack_mixed(mixed)
    psend[0] = tile[0:4]
    psend[1] = tile[4:8]
    psend[2] = pack_square(mixed[40:48], square)[0:4]
    mixed_arrival = exchange(2, 6, psend, precv, 1)

    field_wait(2)
    thrice_w = field_stencil(twice_w, 2)
    put_row(3, thrice_w)
    csend[...] = as_row(row_dots(thrice_w, first_block, second_block, third_block))
    chain_arrival = exchange(3, 7, csend, crecv, 1)
    for x in range(bx):
        for y in range(by):
            out[pl.ds(x * by + y, ROWS, stride=area), :] = t0[x, y]
    back_state = reduce_turn(back_buffers, back_state)

    packed = reduce_end(gram_buffers, gram_state)
    units = [
        jnp.where(lane8 < UNIT,
                  spread(jnp.where(own8, jnp.broadcast_to(packed[u:u + 1], (8, LANES)), 0.0)),
                  0.0)
        for u in range(3)]
    corner = pltpu.roll(jnp.where(lane8 >= 8, units[2], 0.0), 8, 1)
    below = jnp.concatenate(
        [jnp.zeros((8, LANES), f32), jnp.where(lane8 < 8, units[1], 0.0), units[0],
         jnp.zeros((LANES - ROWS, LANES), f32)], axis=0)
    known = jnp.concatenate(
        [jnp.where(lane8 < 8, units[2], 0.0), units[1], units[0] + corner], axis=0)
    known = known + below.T[0:ROWS]
    known = jnp.where((lane < KEEP + 1) & (row < KEEP + 1), known, 0.0)
    norm_sq = jnp.sum(
        jnp.sum(jnp.where((lane == KEEP) & (row == KEEP), known, 0.0), axis=1, keepdims=True),
        axis=0, keepdims=True)
    scale = 1.0 / jnp.maximum(jnp.sqrt(norm_sq), 0.5)
    gram = known * jnp.where(row == KEEP, scale, 1.0) * jnp.where(lane == KEEP, scale, 1.0)
    shifted_row = SHIFT * known[KEEP:KEEP + 1]

    def assemble(form, *extra):
        form = jnp.where(lane1 < KEEP, form, jnp.where(lane1 == KEEP, form * scale, 0.0))
        for at, value in extra:
            form = jnp.where(lane1 == at, value, form)
        return form

    def pick(form, at):
        return jnp.sum(jnp.where(lane1 == at, form, 0.0), axis=1, keepdims=True)

    def column(form, count=2 * ROWS):
        own = row48[0:count] == lane48[0:count]
        return jnp.broadcast_to(
            jnp.sum(jnp.where(own, form, 0.0), axis=1, keepdims=True), (count, LANES))

    def applied(form):
        return pltpu.roll(jnp.where(lane1 < KEEP, form, 0.0), ROWS, 1) + jnp.where(
            (lane1 == KEEP + 1) | (lane1 == KEEP + 2), pltpu.roll(form, 1, 1), 0.0)

    hcols = []

    def arnoldi(rowform, gram, count, last=False):
        c_row = jnp.where(lane1 < count, rowform, 0.0)
        twice = jnp.where(row == lane, 2.0, 0.0) - gram
        t_col = jnp.sum(twice * c_row, axis=1, keepdims=True)
        weights = jnp.broadcast_to(t_col, (ROWS, LANES))
        t_row = jnp.sum(jnp.where(row == lane, weights, 0.0), axis=0, keepdims=True)
        gt_row = jnp.sum(gram * weights, axis=0, keepdims=True)
        length_sq = jnp.sum(
            jnp.where(lane1 == ROWS - 1, rowform, t_row * (gt_row - 2.0 * c_row)),
            axis=1, keepdims=True)
        length_sq = jnp.maximum(length_sq, 0.0)
        length = jnp.sqrt(length_sq)
        inverse = 1.0 / jnp.maximum(length, 0.5)
        hcols.append(jnp.where(lane1 == count, length, t_row))
        if not last:
            e_row = t_row - c_row
            e_col = jnp.sum(jnp.where(row == lane, e_row, 0.0), axis=1, keepdims=True)
            cross_col = (e_col - jnp.sum(gram * e_row, axis=1, keepdims=True)) * inverse
            cross_row = (e_row - jnp.sum(gram * e_col, axis=0, keepdims=True)) * inverse
            corner = length_sq * inverse * inverse
            gram = jnp.where(row == count, cross_row, jnp.where(lane == count, cross_col, gram))
            gram = jnp.where((row == count) & (lane == count), corner, gram)
        return weights, t_row, inverse, gram

    known_row = reduce_end(image_buffers, image_state)
    image_sq = jnp.sum(jnp.where(lane1 == KEEP + 1, known_row, jnp.where(
        lane1 == KEEP, SHIFT * (2.0 * known_row + shifted_row), 0.0)),
        axis=1, keepdims=True) * (scale * scale)
    image_row = (known_row + shifted_row) * scale
    weights, t_row, inverse0, gram1 = arnoldi(
        assemble(image_row, (ROWS - 1, image_sq)), gram, KEEP + 1)
    q21 = assemble(-inverse0 * t_row, (KEEP + 1, scale * inverse0)) + jnp.where(
        lane1 == KEEP, SHIFT * scale * inverse0, 0.0)
    b21 = applied(q21)
    a21 = b21 + SHIFT * q21

    q_square = jnp.where(lane1 < KEEP, q21, 0.0) + jnp.where(
        lane1 == KEEP + 2, pltpu.roll(q21, 2, 1), 0.0)
    q_last = pick(q21, KEEP + 1)
    spread_q = jnp.broadcast_to(q_square, (2 * ROWS, LANES))
    pairs = column(q_square, ROWS) * q_square * jnp.where(lane < row // 8 * 8 + 8, 1.0, 2.0)
    weigh_mixed = pack_mixed(spread_q)
    weigh_square = pack_square(spread_q[0:8], pairs)[0:4]
    weigh_chain = q_last * (2.0 * pltpu.roll(jnp.where(lane1 < KEEP, q21, 0.0), 2 * ROWS, 1)
                            + jnp.where(lane1 == KEEP + 2, 2.0 * q_square, 0.0)
                            + jnp.where(lane1 == KEEP + 3, q_last, 0.0))
    chain_row = gather_sum(chain_arrival, csend[...], crecv)
    chain_sq = jnp.sum(chain_row * weigh_chain, axis=1, keepdims=True)
    total = gather_sum(mixed_arrival, psend[...], precv)
    tile = jnp.concatenate([total[0], total[1]], axis=0) * weigh_mixed
    last = total[2] * weigh_square
    lane4 = lax.broadcasted_iota(jnp.int32, (4, LANES), 1)
    columns = [jnp.sum(jnp.where((lane8 >= ROWS * k) & (lane8 < ROWS * k + ROWS), tile, 0.0),
                       axis=1, keepdims=True) for k in range(5)]
    columns.append(jnp.concatenate([
        jnp.sum(jnp.where(lane4 < ROWS, last, 0.0), axis=1, keepdims=True),
        jnp.zeros((4, 1), f32)], axis=0))
    far_sq = chain_sq + jnp.sum(jnp.sum(
        jnp.where(lane4 < ROWS, 0.0, last), axis=0, keepdims=True), axis=1, keepdims=True)
    own = jnp.where(lane1 < 2 * ROWS, as_row(columns) + q_last * chain_row, 0.0)
    own = jnp.where(lane1 == 2 * ROWS, far_sq, own)
    rsend[...] = own
    row_state = own, exchange(3, 8, rsend, rrecv, 0)

    turn = jnp.where(row < KEEP, -weights, 0.0)
    chain = jnp.where(row8 == 6, (SHIFT - weights[KEEP:KEEP + 1]) * scale,
                      jnp.where(row8 == 7, scale, 0.0))
    far = []
    for x in range(bx):
        dense = jnp.zeros((by, bz), f32)
        for y in range(by):
            at = x * by + y
            v = (turn[0:8] * t2[x, y, 0:8] + turn[8:16] * t2[x, y, 8:16]
                 + (turn[16:24] * t2[x, y, 16:24] + chain * wrow[at * 8:at * 8 + 8]))
            for shift in (4, 2, 1):
                v = v + pltpu.roll(v, shift, 0)
            dense = jnp.where(row3 == y, v, dense)
        far.append(dense)

    def combine(columns, x, y):
        tiles = first_block(x, y) + second_block(x, y)
        terms = [columns[8 * k:8 * k + 8] * tiles[k] for k in range(6)]
        v = (terms[0] + terms[1]) + (terms[2] + terms[3]) + (terms[4] + terms[5])
        for shift in (4, 2, 1):
            v = v + pltpu.roll(v, shift, 0)
        return v

    def field(columns, x):
        dense = jnp.zeros((by, bz), f32)
        for y in range(by):
            dense = jnp.where(row3 == y, combine(columns, x, y), dense)
        return dense

    def put_field(count, x, value):
        out[count * area + x * by:count * area + (x + 1) * by, :] = value

    q21_col = column(q21)
    for x in range(bx):
        put_field(KEEP, x, w_ref[x] * scale)
        put_field(KEEP + 1, x, field(q21_col, x))

    tile = reduce_end(back_buffers, back_state)
    def unpack(at):
        top, source, target, width = places[at]
        return jnp.where((lane8 >= source) & (lane8 < source + width),
                         pltpu.roll(tile, (source - target) % LANES, 1), 0.0)
    square = [unpack(3 + k) for k in range(3)]
    diagonal = [jnp.where(lane8 < ROWS + 8 * (k + 1), square[k], 0.0) for k in range(3)]
    columns = [jnp.where(lane8 == KEEP + 2, pltpu.roll(tile, (KEEP + 2 - 120 - k) % LANES, 1), 0.0)
               for k in range(6)]
    second = jnp.concatenate(columns[0:3], axis=0)
    over = jnp.concatenate([unpack(k) for k in range(3)], axis=0) + jnp.where(
        row < KEEP + 2, second, 0.0)
    strict = jnp.concatenate(
        [over] + [square[k] - diagonal[k] + columns[3 + k] for k in range(3)]
        + [jnp.zeros((LANES - 2 * ROWS, LANES), f32)], axis=0)
    known_col = column(known_row, ROWS)
    known = jnp.where(row == KEEP + 1, jnp.where(lane < KEEP + 2, known_row, 0.0),
                      jnp.where((lane == KEEP + 1) & (row < KEEP + 1), known_col, known))
    whole = jnp.concatenate(
        [known + jnp.where(row == KEEP + 2, second, 0.0)] + diagonal, axis=0)
    whole = whole + strict[0:2 * ROWS] + strict.T[0:2 * ROWS]

    def products(form_col):
        return jnp.sum(whole * form_col, axis=0, keepdims=True)

    y1 = products(column(a21))
    weights, t_row, inverse1, gram2 = arnoldi(
        assemble(y1, (KEEP + 1, jnp.sum(q21 * y1, axis=1, keepdims=True)),
                 (ROWS - 1, jnp.sum(a21 * y1, axis=1, keepdims=True))), gram1, KEEP + 2)
    t_last = pick(t_row, KEEP + 1)
    t_row = assemble(t_row)
    q22 = inverse1 * (a21 - t_row - t_last * q21)
    near = inverse1 * ((SHIFT - t_last) * b21 - applied(t_row)) + SHIFT * q22
    q22_col = column(q22)
    near_col = column(near)
    y_near = products(near_col)
    for x in range(bx):
        put_field(KEEP + 2, x, field(q22_col, x))

    for ref, sem in ((hw, halo_send.at[0]), (hr.at[:, :, :, 0:KEEP], halo_send.at[1]), (gslots, red_send.at[0]),
                     (bslots, red_send.at[1]), (precv, red_send.at[2])):
        pltpu.make_async_copy(ref, ref, sem).wait()

    own = gather_sum(row_state[1], row_state[0], rrecv) * (1.0 / cells)
    y2 = jnp.where(lane1 < 2 * ROWS, y_near + inverse1 * own, 0.0)
    inner = jnp.sum(jnp.concatenate([
        q21 * y2, q22 * y2,
        near * (y2 + inverse1 * own)
        + jnp.where(lane1 == 2 * ROWS, inverse1 * inverse1 * own, 0.0),
        jnp.zeros((5, LANES), f32)], axis=0), axis=1, keepdims=True)
    weights, t_row, inverse2, _ = arnoldi(
        assemble(y2, (KEEP + 1, inner[0:1]), (KEEP + 2, inner[1:2]), (ROWS - 1, inner[2:3])),
        gram2, KEEP + 3, True)
    first = jnp.where(row < KEEP, weights, jnp.where(row == KEEP, weights * scale, 0.0))
    last_col = near_col - jnp.concatenate([first, jnp.zeros((ROWS, LANES), f32)], axis=0)
    last_col = last_col - weights[KEEP + 1:KEEP + 2] * q21_col
    last_col = last_col - weights[KEEP + 2:KEEP + 3] * q22_col
    for x in range(bx):
        put_field(KEEP + 3, x, inverse2 * (field(last_col, x) + inverse1 * inverse0 * far[x]))

    for k in range(EXPAND):
        hess[k:k + 1] = hcols[k]
    pltpu.make_async_copy(rslots, rslots, red_send.at[3]).wait()


def place_results(vectors, columns, out, hess, small, sem):
    large = pltpu.make_async_copy(vectors, out, sem.at[0])
    large.start()
    small[...] = columns[0:EXPAND, 0:ROWS]
    copy = pltpu.make_async_copy(small, hess, sem.at[1])
    copy.start()
    copy.wait()
    large.wait()


def per_device(krylov_basis, schur_vectors, next_vector, diag_shift, velocity):
    sizes = tuple(lax.axis_size(a) for a in AXES)
    block = next_vector.shape
    bx, by, bz = block
    area = bx * by
    basis = krylov_basis.shape[0]
    cells = float(area * bz * sizes[0] * sizes[1] * sizes[2])
    n0, n1 = sizes[1] * sizes[2], sizes[0]
    f32 = jnp.float32
    vmem = pl.BlockSpec(memory_space=pltpu.VMEM)
    dma = pltpu.SemaphoreType.DMA

    vectors, columns = pl.pallas_call(
        functools.partial(body, sizes, cells),
        out_shape=(
            pltpu.VMEM((ROWS * area, bz), f32),
            pltpu.VMEM((8, LANES), f32),
        ),
        in_specs=[
            pl.BlockSpec(memory_space=pl.ANY) for _ in range(5)
        ],
        out_specs=(vmem, vmem),
        scratch_shapes=[
            pltpu.VMEM(schur_vectors.shape[::-1], f32),
            pltpu.VMEM(block, f32),
            pltpu.VMEM(block, f32),
            pltpu.VMEM((3,) + block, f32),
            pltpu.VMEM((basis * PITCH, bz), f32),
            pltpu.VMEM((7,) + block, f32),
            pltpu.VMEM((bx, by, ROWS, bz), f32),
            pltpu.VMEM((bx, by, ROWS, bz), f32),
            pltpu.VMEM((bx, by, ROWS, bz), f32),
            pltpu.VMEM((area * 8, bz), f32),
            pltpu.VMEM((2,) + block, f32),
            pltpu.VMEM((EXPAND, 2, 3, by, bz), f32),
            pltpu.VMEM((2, 2, by + bx + 1, ROWS, bz), f32),
            pltpu.VMEM((EXPAND, 2, 2, by, bz), f32),
            pltpu.VMEM((2, 2, ROWS, bz), f32),
            pltpu.VMEM((128, area * bz), jnp.bfloat16),
            pltpu.VMEM((144, area * bz), jnp.bfloat16),
            pltpu.VMEM((128, area * bz), jnp.bfloat16),
            pltpu.VMEM((2, 3, LANES), f32), pltpu.VMEM((n0 + n1 - 2, 3, LANES), f32),
            pltpu.VMEM((2, 8, LANES), f32), pltpu.VMEM((n0 + n1 - 2, 8, LANES), f32),
            pltpu.VMEM((3, 4, LANES), f32), pltpu.VMEM((n1 - 1, 3, 4, LANES), f32),
            pltpu.VMEM((2, 1, LANES), f32), pltpu.VMEM((1, LANES), f32),
            pltpu.VMEM((1, LANES), f32), pltpu.VMEM((2 * (n0 + n1 - 2), 1, LANES), f32),
            dma((5,)), dma((2,)), dma((5,)), dma((4,)), dma((9,)),
        ],
        compiler_params=pltpu.CompilerParams(collective_id=0, has_side_effects=True),
    )(krylov_basis.reshape(basis, area, bz), schur_vectors.T, next_vector, diag_shift, velocity)
    whole = pl.BlockSpec(memory_space=pl.ANY)
    vectors, columns = pl.pallas_call(
        place_results,
        out_shape=(
            jax.ShapeDtypeStruct((ROWS * area, bz), f32),
            jax.ShapeDtypeStruct((EXPAND, ROWS), f32),
        ),
        in_specs=[vmem, vmem],
        out_specs=(whole, whole),
        scratch_shapes=[pltpu.VMEM((EXPAND, ROWS), f32), dma((2,))],
    )(*(pltpu.with_memory_space_constraint(a, pltpu.VMEM) for a in (vectors, columns)))
    return vectors.reshape((ROWS,) + block), columns.T


def solution(mesh):
    in_specs = (
        P(None, "gx", "gy", "gz"),
        P(),
        P("gx", "gy", "gz"),
        P("gx", "gy", "gz"),
        P(None, "gx", "gy", "gz"),
    )
    out_specs = (P(None, "gx", "gy", "gz"), P())
    return jax.shard_map(
        per_device, mesh=mesh, in_specs=in_specs, out_specs=out_specs, check_vma=False
    )
```

```python
import functools

import jax
import jax.numpy as jnp
from jax import lax
from jax.experimental import pallas as pl
from jax.experimental.pallas import tpu as pltpu
from jax.sharding import PartitionSpec as P

KEEP = 20
EXPAND = 3
ROWS = 24
LANES = 128
UNIT = 16
PITCH = 40
SHIFT = 4.0
AXES = ("gx", "gy", "gz")


def partner_steps(phase, sizes):
    if phase == 1:
        steps = [(dx, 0, 0) for dx in range(1, sizes[0])]
    else:
        steps = [(0, dy, dz) for dy in range(sizes[1]) for dz in range(sizes[2])][1:]
    return sorted(steps, key=lambda step: -sum(
        min(step[d], sizes[d] - step[d]) for d in range(3)))


def body(
    sizes, cells,
    kry_hbm, schur_hbm, w_hbm, diag_hbm, vel_hbm,
    out, hess,
    schur, w_ref, diag, vel, kry, coef, t0, t1, t2, wrow, image,
    hw, hr, faces, zpack, split0, split1, split2,
    gsend, gslots, bsend, bslots, psend, precv, isend, csend, rsend, rslots,
    load_sem, halo_send, halo_recv, red_send, red_recv,
):
    f32, bf16 = jnp.float32, jnp.bfloat16
    place = tuple(lax.axis_index(a) for a in AXES)
    shifted = [[lax.rem(place[d] + k, sizes[d]) for k in range(sizes[d])] for d in range(3)]

    def partners(phase):
        return [tuple(shifted[d][step[d]] for d in range(3))
                for step in partner_steps(phase, sizes)]

    barrier = pltpu.get_barrier_semaphore()
    for to in partners(0) + partners(1):
        pl.semaphore_signal(
            barrier, inc=1, device_id=to, device_id_type=pl.DeviceIdType.MESH)

    basis = kry_hbm.shape[0]
    bx, by, bz = w_ref.shape
    area = bx * by
    loads = [
        pltpu.make_async_copy(source, target, load_sem.at[k])
        for k, (source, target) in enumerate((
            (w_hbm, w_ref), (kry_hbm, kry_hbm), (schur_hbm, schur),
            (diag_hbm, diag), (vel_hbm, vel)))
    ]
    for copy in loads[:1] + loads[2:]:
        copy.start()
    for i in range(basis):
        pltpu.make_async_copy(
            kry_hbm.at[i], kry.at[pl.ds(i * PITCH, area)], load_sem.at[1]).start()
    def halo_copies(sources, targets, send, recv):
        found = []
        for d in range(3):
            for side in (0, 1):
                to = list(place)
                to[d] = shifted[d][1 if side == 0 else sizes[d] - 1]
                found.append(pltpu.make_async_remote_copy(
                    src_ref=sources[d][side], dst_ref=targets[d][side],
                    send_sem=halo_send.at[send], recv_sem=halo_recv.at[recv],
                    device_id=tuple(to), device_id_type=pl.DeviceIdType.MESH,
                ))
        return found

    def halo_start(copies):
        for copy in copies:
            copy.start()

    def field_wait(kind):
        pltpu.make_async_copy(hw.at[kind], hw.at[kind], halo_recv.at[kind]).wait()

    def rows_wait(level):
        landed = hr.at[level, :, :, 0:KEEP]
        pltpu.make_async_copy(landed, landed, halo_recv.at[EXPAND + level]).wait()

    def field_copies(kind, ref):
        return halo_copies(
            ((ref.at[bx - 1], ref.at[0]), (faces.at[kind, 0, 0], faces.at[kind, 1, 0]),
             (faces.at[kind, 0, 1], faces.at[kind, 1, 1])),
            tuple((hw.at[kind, 0, d], hw.at[kind, 1, d]) for d in range(3)), 0, kind)

    def rows_copies(level, ref):
        return halo_copies(
            ((ref.at[bx - 1, :, 0:KEEP], ref.at[0, :, 0:KEEP]),
             (ref.at[:, by - 1, 0:KEEP], ref.at[:, 0, 0:KEEP]),
             (zpack.at[level, 0, 0:KEEP], zpack.at[level, 1, 0:KEEP])),
            tuple((hr.at[level, 0, part, 0:KEEP], hr.at[level, 1, part, 0:KEEP])
                  for part in (pl.ds(0, by), pl.ds(by, bx), by + bx)), 1, EXPAND + level)

    def exchange(kind, at, send, slots, phase):
        for k, to in enumerate(partners(phase)):
            pltpu.make_async_remote_copy(
                src_ref=send, dst_ref=slots.at[k], send_sem=red_send.at[kind],
                recv_sem=red_recv.at[at],
                device_id=to, device_id_type=pl.DeviceIdType.MESH,
            ).start()
        return pltpu.make_async_copy(slots, slots, red_recv.at[at])

    def gather_sum(arrival, own, slots):
        arrival.wait()
        terms = [own] + [slots[k] for k in range(slots.shape[0])]
        while len(terms) > 1:
            terms = [sum(terms[k + 1:k + 2], terms[k]) for k in range(0, len(terms), 2)]
        return terms[0]

    def reduce_start(buffers, value):
        kind, at, send, slots0, _ = buffers
        send[0] = value
        return value, exchange(kind, at, send.at[0], slots0, 0)

    def reduce_turn(buffers, state):
        kind, at, send, slots0, slots1 = buffers
        value = gather_sum(state[1], state[0], slots0)
        send[1] = value
        return value, exchange(kind, at + 1, send.at[1], slots1, 1)

    def reduce_end(buffers, state):
        return gather_sum(state[1], state[0], buffers[4]) * (1.0 / cells)

    n0, n1 = len(partner_steps(0, sizes)), len(partner_steps(1, sizes))
    gram_buffers = (0, 0, gsend, gslots.at[pl.ds(0, n0)], gslots.at[pl.ds(n0, n1)])
    back_buffers = (1, 2, bsend, bslots.at[pl.ds(0, n0)], bslots.at[pl.ds(n0, n1)])
    image_buffers = (3, 4, isend, rslots.at[pl.ds(0, n0)], rslots.at[pl.ds(n0, n1)])
    crecv = rslots.at[pl.ds(n0 + n1, n1)]
    rrecv = rslots.at[pl.ds(n0 + 2 * n1, n0)]

    lane3 = lax.broadcasted_iota(jnp.int32, (by, bz), 1)
    row3 = lax.broadcasted_iota(jnp.int32, (by, bz), 0)
    lane24 = lax.broadcasted_iota(jnp.int32, (ROWS, bz), 1)

    def field_stencil(v, kind):
        res = []
        for x in range(bx):
            here = v[x]
            xb = v[x - 1] if x > 0 else hw[kind, 0, 0]
            xa = v[x + 1] if x < bx - 1 else hw[kind, 1, 0]
            yb = jnp.where(row3 == 0, hw[kind, 0, 1, x:x + 1, :], pltpu.roll(here, 1, 0))
            ya = jnp.where(row3 == by - 1, hw[kind, 1, 1, x:x + 1, :], pltpu.roll(here, by - 1, 0))
            zb = jnp.where(lane3 == 0, hw[kind, 0, 2, :, x:x + 1], pltpu.roll(here, 1, 1))
            za = jnp.where(lane3 == bz - 1, hw[kind, 1, 2, :, x:x + 1], pltpu.roll(here, bz - 1, 1))
            res.append(coef[6, x] * here + (coef[0, x] * xb + coef[1, x] * xa)
                       + (coef[2, x] * yb + coef[3, x] * ya)
                       + (coef[4, x] * zb + coef[5, x] * za))
        return res

    inner = [(x, y) for x in range(1, bx - 1) for y in range(1, by - 1)]
    outer = [(x, y) for x in range(bx) for y in range(by) if (x, y) not in inner]

    def rows_stencil(level, source, target, where):
        low, high = hr[level, 0, by + bx], hr[level, 1, by + bx]
        for x, y in where:
            at = x * by + y
            here = source[x, y]
            xb = source[x - 1, y] if x > 0 else hr[level, 0, y]
            xa = source[x + 1, y] if x < bx - 1 else hr[level, 1, y]
            yb = source[x, y - 1] if y > 0 else hr[level, 0, by + x]
            ya = source[x, y + 1] if y < by - 1 else hr[level, 1, by + x]
            zb = jnp.where(lane24 == 0, pltpu.roll(low, (bz - at) % bz, 1),
                           pltpu.roll(here, 1, 1))
            za = jnp.where(lane24 == bz - 1, pltpu.roll(high, bz - 1 - at, 1),
                           pltpu.roll(here, bz - 1, 1))
            c = [coef[k, x, y:y + 1, :] for k in range(7)]
            target[x, y] = (c[6] * here + (c[0] * xb + c[1] * xa)
                            + (c[2] * yb + c[3] * ya) + (c[4] * zb + c[5] * za))

    def pack_ends(kind, tiles):
        for side, (near, edge) in enumerate(((by - 1, bz - 1), (0, 0))):
            rows = jnp.zeros((by, bz), f32)
            lanes = jnp.zeros((by, bz), f32)
            for x in range(bx):
                rows = jnp.where(row3 == x, pltpu.roll(tiles[x], (x - near) % by, 0), rows)
                lanes = jnp.where(lane3 == x, pltpu.roll(tiles[x], (x - edge) % bz, 1), lanes)
            faces[kind, side, 0] = rows
            faces[kind, side, 1] = lanes

    def pack_faces(level, source):
        for side, edge in enumerate((bz - 1, 0)):
            face = jnp.zeros((ROWS, bz), f32)
            for x in range(bx):
                for y in range(by):
                    at = x * by + y
                    face = jnp.where(
                        lane24 == at, pltpu.roll(source[x, y], (at - edge) % bz, 1), face)
            zpack[level, side] = face

    def put_row(k, tiles):
        for x in range(bx):
            wrow[pl.ds(x * by * 8 + 4 + k, by, stride=8), :] = tiles[x]

    def tail(x, y):
        return t0[x, y, 16:24] + wrow[(x * by + y) * 8:(x * by + y) * 8 + 8]

    def first_block(x, y):
        return [t0[x, y, 0:8], t0[x, y, 8:16], tail(x, y)]

    def second_block(x, y):
        return [t1[x, y, 0:8], t1[x, y, 8:16], t1[x, y, 16:24]]

    def third_block(x, y):
        return [t2[x, y, 0:8], t2[x, y, 8:16], t2[x, y, 16:24]]

    def row_dots(tiles, *blocks):
        sums = [jnp.zeros((8, bz), f32) for _ in range(3 * len(blocks))]
        for x in range(bx):
            for y in range(by):
                v = jnp.broadcast_to(tiles[x][y:y + 1, :], (8, bz))
                for k, part in enumerate([t for block in blocks for t in block(x, y)]):
                    sums[k] = sums[k] + part * v
        return [jnp.sum(total, axis=1, keepdims=True) for total in sums]

    def as_row(columns):
        count = 8 * len(columns)
        own = (lax.broadcasted_iota(jnp.int32, (count, LANES), 0)
               == lax.broadcasted_iota(jnp.int32, (count, LANES), 1))
        return jnp.sum(jnp.where(own, jnp.concatenate(columns, axis=0), 0.0), axis=0, keepdims=True)

    def put_split(ref, p, u, first=0, pitch=None):
        n = u.shape[0]
        pitch = pitch or n
        at = pl.ds(p * 2 * bz, 2 * bz)
        high = u.astype(bf16)
        rest = u - high.astype(f32)
        mid = rest.astype(bf16)
        ref[first:first + n, at] = high
        ref[first + pitch:first + pitch + n, at] = mid
        ref[first + 2 * pitch:first + 2 * pitch + n, at] = (rest - mid.astype(f32)).astype(bf16)

    def both(block, p):
        return [jnp.concatenate([block(*divmod(2 * p, by))[k], block(*divmod(2 * p + 1, by))[k]],
                                axis=1) for k in range(3)]

    dot_nt = functools.partial(
        lax.dot_general, dimension_numbers=(((1,), (1,)), ((), ())), preferred_element_type=f32)

    row = lax.broadcasted_iota(jnp.int32, (ROWS, LANES), 0)
    lane = lax.broadcasted_iota(jnp.int32, (ROWS, LANES), 1)
    lane1 = lax.broadcasted_iota(jnp.int32, (1, LANES), 1)
    row8 = lax.broadcasted_iota(jnp.int32, (8, LANES), 0)
    lane8 = lax.broadcasted_iota(jnp.int32, (8, LANES), 1)
    row48 = lax.broadcasted_iota(jnp.int32, (2 * ROWS, LANES), 0)
    lane48 = lax.broadcasted_iota(jnp.int32, (2 * ROWS, LANES), 1)

    halo_w = field_copies(0, w_ref)
    wrow[...] = jnp.zeros_like(wrow)
    hr[:, :, :, KEEP:ROWS] = jnp.zeros(hr.shape[0:3] + (ROWS - KEEP, bz), f32)
    t0[:, :, 16:24] = jnp.zeros((bx, by, 8, bz), f32)
    split0[96:128] = jnp.zeros((32, split0.shape[1]), bf16)
    split2[96:128] = jnp.zeros((32, split2.shape[1]), bf16)

    loads[2].wait()
    loads[1].wait()
    turn = schur[...]
    turn_high = turn.astype(bf16)
    turn_low = (turn - turn_high.astype(f32)).astype(bf16)
    for p in range(area // 2):
        u = jnp.concatenate([kry[pl.ds(2 * p, basis, stride=PITCH), :],
                             kry[pl.ds(2 * p + 1, basis, stride=PITCH), :]], axis=1)
        high = u.astype(bf16)
        low = (u - high.astype(f32)).astype(bf16)
        r = (jnp.dot(turn_high, high, preferred_element_type=f32)
             + (jnp.dot(turn_high, low, preferred_element_type=f32)
                + jnp.dot(turn_low, high, preferred_element_type=f32)))
        for k in (0, 1):
            x, y = divmod(2 * p + k, by)
            t0[x, y, 0:KEEP] = r[:, k * bz:(k + 1) * bz]
    pack_faces(0, t0)
    halo_r = rows_copies(0, t0)
    loads[0].wait()
    w = [w_ref[x] for x in range(bx)]
    pack_ends(0, w)
    put_row(0, w)
    pl.semaphore_wait(barrier, len(partners(0)) + len(partners(1)))
    halo_start(halo_w)
    halo_start(halo_r)

    loads[3].wait()
    loads[4].wait()
    for x in range(bx):
        for d in range(3):
            half = 0.5 * vel[d, x]
            at = (x, row3, lane3)[d]
            span = (bx, by, bz)[d]
            coef[2 * d, x] = jnp.where((at == 0) & (place[d] == 0), 0.0, -1.0 - half)
            coef[2 * d + 1, x] = jnp.where(
                (at == span - 1) & (place[d] == sizes[d] - 1), 0.0, half - 1.0)
        coef[6, x] = (6.0 - SHIFT) + diag[x]
    zero8 = jnp.zeros((8, 2 * bz), f32)
    for p in range(area // 2):
        put_split(split0, p, jnp.concatenate(both(first_block, p) + [zero8], axis=0))
    prod = dot_nt(split0[0:96], split0[...])
    prod = prod[0:24] + prod[32:56] + prod[64:88]
    gram = prod + pltpu.roll(prod, LANES - 32, 1) + pltpu.roll(prod, LANES - 64, 1)

    own8 = lane8 // UNIT == row8

    def spread(value):
        for shift in (UNIT, 2 * UNIT, 4 * UNIT):
            value = value + pltpu.roll(value, shift, 1)
        return value

    units = (
        gram[16:24],
        gram[8:16],
        jnp.where(lane8 < 8, gram[0:8], pltpu.roll(gram[16:24], LANES - 8, 1)),
    )
    packed = jnp.concatenate([
        jnp.sum(jnp.where(own8, spread(jnp.where(lane8 < UNIT, unit, 0.0)), 0.0),
                axis=0, keepdims=True)
        for unit in units], axis=0)
    gram_state = reduce_start(gram_buffers, packed)

    field_wait(0)
    once = field_stencil(w, 0)
    for x in range(bx):
        image[0, x] = once[x]
    pack_ends(1, once)
    halo_a = field_copies(1, image.at[0])
    halo_start(halo_a)
    own = as_row(row_dots(once, first_block))
    squares = sum((tile * tile for tile in once[1:]), once[0] * once[0])
    own = jnp.where(lane1 == KEEP + 1, jnp.sum(
        jnp.sum(squares, axis=0, keepdims=True), axis=1, keepdims=True), own)
    image_state = reduce_start(image_buffers, own)
    put_row(1, once)

    rows_wait(0)
    halo_t = rows_copies(1, t1)
    rows_stencil(0, t0, t1, outer)
    halo_start(halo_t[0:4])
    rows_stencil(0, t0, t1, inner)
    pack_faces(1, t1)
    halo_start(halo_t[4:6])
    for p in range(area // 2):
        put_split(split1, p, jnp.concatenate(
            both(first_block, p) + both(second_block, p), axis=0))
    prod = dot_nt(split1[...], split1[...])
    prod = prod[0:48] + prod[48:96] + prod[96:144]
    left = prod[:, 0:LANES]
    right = jnp.concatenate(
        [prod[:, LANES:], jnp.zeros((48, 2 * LANES - prod.shape[1]), f32)], axis=1)
    cross = left + pltpu.roll(left, LANES - 48, 1) + jnp.where(
        lane48 < 32, pltpu.roll(left, LANES - 96, 1), pltpu.roll(right, 32, 1))

    field_wait(1)
    twice_w = field_stencil(once, 1)
    for x in range(bx):
        image[1, x] = twice_w[x]
    pack_ends(2, twice_w)
    halo_b = field_copies(2, image.at[1])
    halo_start(halo_b)
    put_row(2, twice_w)

    places = ((0, 24, 0, 24), (8, 24, 24, 24), (16, 24, 48, 24), (24, 24, 72, 24),
              (32, 32, 96, 16), (40, 40, 112, 8))
    tile = jnp.zeros((8, LANES), f32)
    for top, source, target, width in places:
        tile = jnp.where((lane8 >= target) & (lane8 < target + width),
                         pltpu.roll(cross[top:top + 8], (target - source) % LANES, 1), tile)
    for k, col in enumerate(row_dots(twice_w, first_block, second_block)):
        tile = jnp.where(lane8 == 120 + k, col, tile)
    back_state = reduce_start(back_buffers, tile)
    for p in range(area // 2):
        put_split(split1, p, jnp.concatenate(
            both(first_block, p)[2:3] + both(second_block, p)[0:1], axis=0), 16, 2 * ROWS)

    rows_wait(1)
    rows_stencil(1, t1, t2, outer + inner)
    def third_tail(x, y):
        return third_block(x, y)[0:2] + [t2[x, y, 16:24]
                                         + wrow[(x * by + y) * 8:(x * by + y) * 8 + 8]]
    for p in range(area // 2):
        put_split(split2, p, jnp.concatenate(both(third_tail, p) + [zero8], axis=0))

    def fold(prod):
        return prod + pltpu.roll(prod, LANES - 32, 1) + pltpu.roll(prod, LANES - 64, 1)

    prod = dot_nt(split1[...], split2[...])
    mixed = fold(prod[0:48] + prod[48:96] + prod[96:144])
    prod = dot_nt(split2[0:96], split2[...])
    square = fold(prod[0:24] + prod[32:56] + prod[64:88])

    def pack_mixed(value):
        tile = jnp.zeros((8, LANES), f32)
        for k in range(5):
            tile = jnp.where((lane8 >= ROWS * k) & (lane8 < ROWS * k + ROWS),
                             pltpu.roll(value[8 * k:8 * k + 8], ROWS * k, 1), tile)
        return tile

    def pack_square(last, value):
        tile = jnp.where(lane8 < ROWS, last, 0.0)
        start = ROWS
        for k in range(3):
            width = ROWS - 8 * k
            for half in (0, 1):
                part = value[8 * k:8 * k + 8]
                if half:
                    part = pltpu.roll(part, 4, 0)
                tile = jnp.where((lane8 >= start) & (lane8 < start + width),
                                 pltpu.roll(part, (start - 8 * k) % LANES, 1), tile)
                start = start + width
        return tile

    gram_state = reduce_turn(gram_buffers, gram_state)
    image_state = reduce_turn(image_buffers, image_state)
    tile = pack_mixed(mixed)
    psend[0] = tile[0:4]
    psend[1] = tile[4:8]
    psend[2] = pack_square(mixed[40:48], square)[0:4]
    mixed_arrival = exchange(2, 6, psend, precv, 1)

    field_wait(2)
    thrice_w = field_stencil(twice_w, 2)
    put_row(3, thrice_w)
    csend[...] = as_row(row_dots(thrice_w, first_block, second_block, third_block))
    chain_arrival = exchange(3, 7, csend, crecv, 1)
    for x in range(bx):
        for y in range(by):
            out[pl.ds(x * by + y, ROWS, stride=area), :] = t0[x, y]
    back_state = reduce_turn(back_buffers, back_state)

    packed = reduce_end(gram_buffers, gram_state)
    units = [
        jnp.where(lane8 < UNIT,
                  spread(jnp.where(own8, jnp.broadcast_to(packed[u:u + 1], (8, LANES)), 0.0)),
                  0.0)
        for u in range(3)]
    corner = pltpu.roll(jnp.where(lane8 >= 8, units[2], 0.0), 8, 1)
    below = jnp.concatenate(
        [jnp.zeros((8, LANES), f32), jnp.where(lane8 < 8, units[1], 0.0), units[0],
         jnp.zeros((LANES - ROWS, LANES), f32)], axis=0)
    known = jnp.concatenate(
        [jnp.where(lane8 < 8, units[2], 0.0), units[1], units[0] + corner], axis=0)
    known = known + below.T[0:ROWS]
    known = jnp.where((lane < KEEP + 1) & (row < KEEP + 1), known, 0.0)
    norm_sq = jnp.sum(
        jnp.sum(jnp.where((lane == KEEP) & (row == KEEP), known, 0.0), axis=1, keepdims=True),
        axis=0, keepdims=True)
    scale = 1.0 / jnp.maximum(jnp.sqrt(norm_sq), 0.5)
    gram = known * jnp.where(row == KEEP, scale, 1.0) * jnp.where(lane == KEEP, scale, 1.0)
    shifted_row = SHIFT * known[KEEP:KEEP + 1]

    def assemble(form, *extra):
        form = jnp.where(lane1 < KEEP, form, jnp.where(lane1 == KEEP, form * scale, 0.0))
        for at, value in extra:
            form = jnp.where(lane1 == at, value, form)
        return form

    def pick(form, at):
        return jnp.sum(jnp.where(lane1 == at, form, 0.0), axis=1, keepdims=True)

    def column(form, count=2 * ROWS):
        own = row48[0:count] == lane48[0:count]
        return jnp.broadcast_to(
            jnp.sum(jnp.where(own, form, 0.0), axis=1, keepdims=True), (count, LANES))

    def applied(form):
        return pltpu.roll(jnp.where(lane1 < KEEP, form, 0.0), ROWS, 1) + jnp.where(
            (lane1 == KEEP + 1) | (lane1 == KEEP + 2), pltpu.roll(form, 1, 1), 0.0)

    hcols = []

    def arnoldi(rowform, gram, count, last=False):
        c_row = jnp.where(lane1 < count, rowform, 0.0)
        twice = jnp.where(row == lane, 2.0, 0.0) - gram
        t_col = jnp.sum(twice * c_row, axis=1, keepdims=True)
        weights = jnp.broadcast_to(t_col, (ROWS, LANES))
        t_row = jnp.sum(jnp.where(row == lane, weights, 0.0), axis=0, keepdims=True)
        gt_row = jnp.sum(gram * weights, axis=0, keepdims=True)
        length_sq = jnp.sum(
            jnp.where(lane1 == ROWS - 1, rowform, t_row * (gt_row - 2.0 * c_row)),
            axis=1, keepdims=True)
        length_sq = jnp.maximum(length_sq, 0.0)
        length = jnp.sqrt(length_sq)
        inverse = 1.0 / jnp.maximum(length, 0.5)
        hcols.append(jnp.where(lane1 == count, length, t_row))
        if not last:
            e_row = t_row - c_row
            e_col = jnp.sum(jnp.where(row == lane, e_row, 0.0), axis=1, keepdims=True)
            cross_col = (e_col - jnp.sum(gram * e_row, axis=1, keepdims=True)) * inverse
            cross_row = (e_row - jnp.sum(gram * e_col, axis=0, keepdims=True)) * inverse
            corner = length_sq * inverse * inverse
            gram = jnp.where(row == count, cross_row, jnp.where(lane == count, cross_col, gram))
            gram = jnp.where((row == count) & (lane == count), corner, gram)
        return weights, t_row, inverse, gram

    known_row = reduce_end(image_buffers, image_state)
    image_sq = jnp.sum(jnp.where(lane1 == KEEP + 1, known_row, jnp.where(
        lane1 == KEEP, SHIFT * (2.0 * known_row + shifted_row), 0.0)),
        axis=1, keepdims=True) * (scale * scale)
    image_row = (known_row + shifted_row) * scale
    weights, t_row, inverse0, gram1 = arnoldi(
        assemble(image_row, (ROWS - 1, image_sq)), gram, KEEP + 1)
    q21 = assemble(-inverse0 * t_row, (KEEP + 1, scale * inverse0)) + jnp.where(
        lane1 == KEEP, SHIFT * scale * inverse0, 0.0)
    b21 = applied(q21)
    a21 = b21 + SHIFT * q21

    q_square = jnp.where(lane1 < KEEP, q21, 0.0) + jnp.where(
        lane1 == KEEP + 2, pltpu.roll(q21, 2, 1), 0.0)
    q_last = pick(q21, KEEP + 1)
    spread_q = jnp.broadcast_to(q_square, (2 * ROWS, LANES))
    pairs = column(q_square, ROWS) * q_square * jnp.where(lane < row // 8 * 8 + 8, 1.0, 2.0)
    weigh_mixed = pack_mixed(spread_q)
    weigh_square = pack_square(spread_q[0:8], pairs)[0:4]
    weigh_chain = q_last * (2.0 * pltpu.roll(jnp.where(lane1 < KEEP, q21, 0.0), 2 * ROWS, 1)
                            + jnp.where(lane1 == KEEP + 2, 2.0 * q_square, 0.0)
                            + jnp.where(lane1 == KEEP + 3, q_last, 0.0))
    total = gather_sum(mixed_arrival, psend[...], precv)
    tile = jnp.concatenate([total[0], total[1]], axis=0) * weigh_mixed
    last = total[2] * weigh_square
    lane4 = lax.broadcasted_iota(jnp.int32, (4, LANES), 1)
    columns = [jnp.sum(jnp.where((lane8 >= ROWS * k) & (lane8 < ROWS * k + ROWS), tile, 0.0),
                       axis=1, keepdims=True) for k in range(5)]
    columns.append(jnp.concatenate([
        jnp.sum(jnp.where(lane4 < ROWS, last, 0.0), axis=1, keepdims=True),
        jnp.zeros((4, 1), f32)], axis=0))
    own = jnp.where(lane1 == 2 * ROWS, jnp.sum(jnp.sum(
        jnp.where(lane4 < ROWS, 0.0, last), axis=0, keepdims=True), axis=1, keepdims=True),
        as_row(columns))
    chain_row = gather_sum(chain_arrival, csend[...], crecv)
    own = own + jnp.where(
        lane1 == 2 * ROWS, jnp.sum(chain_row * weigh_chain, axis=1, keepdims=True),
        jnp.where(lane1 < 2 * ROWS, q_last * chain_row, 0.0))
    rsend[...] = own
    row_state = own, exchange(3, 8, rsend, rrecv, 0)

    turn = jnp.where(row < KEEP, -weights, 0.0)
    chain = jnp.where(row8 == 6, (SHIFT - weights[KEEP:KEEP + 1]) * scale,
                      jnp.where(row8 == 7, scale, 0.0))
    far = []
    for x in range(bx):
        dense = jnp.zeros((by, bz), f32)
        for y in range(by):
            at = x * by + y
            v = (turn[0:8] * t2[x, y, 0:8] + turn[8:16] * t2[x, y, 8:16]
                 + (turn[16:24] * t2[x, y, 16:24] + chain * wrow[at * 8:at * 8 + 8]))
            for shift in (4, 2, 1):
                v = v + pltpu.roll(v, shift, 0)
            dense = jnp.where(row3 == y, v, dense)
        far.append(dense)

    def combine(columns, x, y):
        tiles = first_block(x, y)
        if columns.shape[0] > ROWS:
            tiles = tiles + second_block(x, y)
        terms = [columns[8 * k:8 * k + 8] * tile for k, tile in enumerate(tiles)]
        v = sum(terms[1:], terms[0])
        for shift in (4, 2, 1):
            v = v + pltpu.roll(v, shift, 0)
        return v

    def field(columns, x):
        dense = jnp.zeros((by, bz), f32)
        for y in range(by):
            dense = jnp.where(row3 == y, combine(columns, x, y), dense)
        return dense

    def put_field(count, x, value):
        out[count * area + x * by:count * area + (x + 1) * by, :] = value

    q21_col = column(q21)
    for x in range(bx):
        put_field(KEEP, x, w_ref[x] * scale)
        put_field(KEEP + 1, x, field(q21_col, x))

    tile = reduce_end(back_buffers, back_state)
    def unpack(at):
        top, source, target, width = places[at]
        return jnp.where((lane8 >= source) & (lane8 < source + width),
                         pltpu.roll(tile, (source - target) % LANES, 1), 0.0)
    square = [unpack(3 + k) for k in range(3)]
    diagonal = [jnp.where(lane8 < ROWS + 8 * (k + 1), square[k], 0.0) for k in range(3)]
    columns = [jnp.where(lane8 == KEEP + 2, pltpu.roll(tile, (KEEP + 2 - 120 - k) % LANES, 1), 0.0)
               for k in range(6)]
    second = jnp.concatenate(columns[0:3], axis=0)
    over = jnp.concatenate([unpack(k) for k in range(3)], axis=0) + jnp.where(
        row < KEEP + 2, second, 0.0)
    strict = jnp.concatenate(
        [over] + [square[k] - diagonal[k] + columns[3 + k] for k in range(3)]
        + [jnp.zeros((LANES - 2 * ROWS, LANES), f32)], axis=0)
    known_col = column(known_row, ROWS)
    known = jnp.where(row == KEEP + 1, jnp.where(lane < KEEP + 2, known_row, 0.0),
                      jnp.where((lane == KEEP + 1) & (row < KEEP + 1), known_col, known))
    whole = jnp.concatenate(
        [known + jnp.where(row == KEEP + 2, second, 0.0)] + diagonal, axis=0)
    whole = whole + strict[0:2 * ROWS] + strict.T[0:2 * ROWS]

    def products(form_col):
        return jnp.sum(whole * form_col, axis=0, keepdims=True)

    y1 = products(column(a21))
    weights, t_row, inverse1, gram2 = arnoldi(
        assemble(y1, (KEEP + 1, jnp.sum(q21 * y1, axis=1, keepdims=True)),
                 (ROWS - 1, jnp.sum(a21 * y1, axis=1, keepdims=True))), gram1, KEEP + 2)
    t_last = pick(t_row, KEEP + 1)
    t_row = assemble(t_row)
    q22 = inverse1 * (a21 - t_row - t_last * q21)
    near = inverse1 * ((SHIFT - t_last) * b21 - applied(t_row)) + SHIFT * q22
    q22_col = column(q22)
    near_col = column(near)
    y_near = products(near_col)
    for x in range(bx):
        put_field(KEEP + 2, x, field(q22_col, x))
    base = [field(near_col, x) + inverse1 * inverse0 * far[x] for x in range(bx)]

    for ref, sem in ((hw, halo_send.at[0]), (hr.at[:, :, :, 0:KEEP], halo_send.at[1]), (gslots, red_send.at[0]),
                     (bslots, red_send.at[1]), (precv, red_send.at[2])):
        pltpu.make_async_copy(ref, ref, sem).wait()

    own = gather_sum(row_state[1], row_state[0], rrecv) * (1.0 / cells)
    y2 = jnp.where(lane1 < 2 * ROWS, y_near + inverse1 * own, 0.0)
    inner = jnp.sum(jnp.concatenate([
        q21 * y2, q22 * y2,
        near * (y2 + inverse1 * own)
        + jnp.where(lane1 == 2 * ROWS, inverse1 * inverse1 * own, 0.0),
        jnp.zeros((5, LANES), f32)], axis=0), axis=1, keepdims=True)
    weights, t_row, inverse2, _ = arnoldi(
        assemble(y2, (KEEP + 1, inner[0:1]), (KEEP + 2, inner[1:2]), (ROWS - 1, inner[2:3])),
        gram2, KEEP + 3, True)
    first = jnp.where(row < KEEP, weights, jnp.where(row == KEEP, weights * scale, 0.0))
    for x in range(bx):
        value = base[x] - field(first, x)
        for count in (KEEP + 1, KEEP + 2):
            at = count * area + x * by
            value = value - weights[count:count + 1] * out[at:at + by, :]
        put_field(KEEP + 3, x, inverse2 * value)

    for k in range(EXPAND):
        hess[k:k + 1] = hcols[k]
    pltpu.make_async_copy(rslots, rslots, red_send.at[3]).wait()


def place_results(vectors, columns, out, hess, small, sem):
    large = pltpu.make_async_copy(vectors, out, sem.at[0])
    large.start()
    small[...] = columns[0:EXPAND, 0:ROWS]
    copy = pltpu.make_async_copy(small, hess, sem.at[1])
    copy.start()
    copy.wait()
    large.wait()


def per_device(krylov_basis, schur_vectors, next_vector, diag_shift, velocity):
    sizes = tuple(lax.axis_size(a) for a in AXES)
    block = next_vector.shape
    bx, by, bz = block
    area = bx * by
    basis = krylov_basis.shape[0]
    cells = float(area * bz * sizes[0] * sizes[1] * sizes[2])
    n0, n1 = sizes[1] * sizes[2], sizes[0]
    f32 = jnp.float32
    vmem = pl.BlockSpec(memory_space=pltpu.VMEM)
    dma = pltpu.SemaphoreType.DMA

    vectors, columns = pl.pallas_call(
        functools.partial(body, sizes, cells),
        out_shape=(
            pltpu.VMEM((ROWS * area, bz), f32),
            pltpu.VMEM((8, LANES), f32),
        ),
        in_specs=[
            pl.BlockSpec(memory_space=pl.ANY) for _ in range(5)
        ],
        out_specs=(vmem, vmem),
        scratch_shapes=[
            pltpu.VMEM(schur_vectors.shape[::-1], f32),
            pltpu.VMEM(block, f32),
            pltpu.VMEM(block, f32),
            pltpu.VMEM((3,) + block, f32),
            pltpu.VMEM((-(-basis // 8) * 8 * PITCH, bz), f32),
            pltpu.VMEM((7,) + block, f32),
            pltpu.VMEM((bx, by, ROWS, bz), f32),
            pltpu.VMEM((bx, by, ROWS, bz), f32),
            pltpu.VMEM((bx, by, ROWS, bz), f32),
            pltpu.VMEM((area * 8, bz), f32),
            pltpu.VMEM((2,) + block, f32),
            pltpu.VMEM((EXPAND, 2, 3, by, bz), f32),
            pltpu.VMEM((2, 2, by + bx + 1, ROWS, bz), f32),
            pltpu.VMEM((EXPAND, 2, 2, by, bz), f32),
            pltpu.VMEM((2, 2, ROWS, bz), f32),
            pltpu.VMEM((128, area * bz), jnp.bfloat16),
            pltpu.VMEM((144, area * bz), jnp.bfloat16),
            pltpu.VMEM((128, area * bz), jnp.bfloat16),
            pltpu.VMEM((2, 3, LANES), f32), pltpu.VMEM((n0 + n1 - 2, 3, LANES), f32),
            pltpu.VMEM((2, 8, LANES), f32), pltpu.VMEM((n0 + n1 - 2, 8, LANES), f32),
            pltpu.VMEM((3, 4, LANES), f32), pltpu.VMEM((n1 - 1, 3, 4, LANES), f32),
            pltpu.VMEM((2, 1, LANES), f32), pltpu.VMEM((1, LANES), f32),
            pltpu.VMEM((1, LANES), f32), pltpu.VMEM((2 * (n0 + n1 - 2), 1, LANES), f32),
            dma((5,)), dma((2,)), dma((5,)), dma((4,)), dma((9,)),
        ],
        compiler_params=pltpu.CompilerParams(collective_id=0, has_side_effects=True),
    )(krylov_basis.reshape(basis, area, bz), schur_vectors.T, next_vector, diag_shift, velocity)
    whole = pl.BlockSpec(memory_space=pl.ANY)
    vectors, columns = pl.pallas_call(
        place_results,
        out_shape=(
            jax.ShapeDtypeStruct((ROWS * area, bz), f32),
            jax.ShapeDtypeStruct((EXPAND, ROWS), f32),
        ),
        in_specs=[vmem, vmem],
        out_specs=(whole, whole),
        scratch_shapes=[pltpu.VMEM((EXPAND, ROWS), f32), dma((2,))],
    )(*(pltpu.with_memory_space_constraint(a, pltpu.VMEM) for a in (vectors, columns)))
    return vectors.reshape((ROWS,) + block), columns.T


def solution(mesh):
    in_specs = (
        P(None, "gx", "gy", "gz"),
        P(),
        P("gx", "gy", "gz"),
        P("gx", "gy", "gz"),
        P(None, "gx", "gy", "gz"),
    )
    out_specs = (P(None, "gx", "gy", "gz"), P())
    return jax.shard_map(
        per_device, mesh=mesh, in_specs=in_specs, out_specs=out_specs, check_vma=False
    )
```
